32 devices in a mesh: gx: 2 (over x), gy: 4 (over y, core), gz: 4 (over z).
Axes of the slice: x: 2, y: 2, z: 4, core: 2. Of those that a mesh axis runs over, the one named last changes fastest.
Arguments:
- metric_pert: float32 [6, 32, 64, 512], P(None, 'gx', 'gy', 'gz'), may hold values from -1.8 to 1.8
- curvature: float32 [6, 32, 64, 512], P(None, 'gx', 'gy', 'gz'), may hold values from -6 to 6
- interp_weights: bfloat16 [2, 4, 32, 64, 4096], P('gx', 'gy', 'gz'), may hold values from -0.09375 to 0.09375
- point_ids: int32 [2, 4, 32, 64], P('gx', 'gy', 'gz'), may hold values from 0 to 6144, as said below
- theta: float32 [6144], replicated, may hold values from 0.05 to 3.09
- phi: float32 [6144], replicated, may hold values from -3.140625 to 3.140625
Outputs:
- psi4_field: bfloat16 [2, 32, 64, 512], P(None, 'gx', 'gy', 'gz')
- modes: float32 [3, 2, 77], replicated
The draws below stay inside these ranges and needn't reach their ends.
Inputs may be any that keep to these rules, and one draw needn't show every extreme that they name: `point_ids`: the grid is a window of the extraction region that the spheres cross. A live entry names a sphere point; the value 6144 marks an empty slot, and each list holds its live entries first. The points of sphere s lie in the 9 consecutive block layers along the third dimension that begin at layer s * 10; each point belongs to one column (bx, by) and is listed in exactly two blocks of that column that are adjacent along the third dimension. Some block's list is full, every listing block holds at least 32 live entries, and blocks outside these layers list no point.
All inputs are finite; a program needn't handle non-finite values.
Results may differ from the reference program's by a relative error of at most 0.0032.
Values sent between devices are 32-bit elements; how exact they have to be, the bound alone decides.
A program may use at most 64 MiB of HBM per device.

```python
import math
import jax
import jax.numpy as jnp
import numpy as np
from jax import lax

BLK = 16
PB = 64
PTS = 2048
SPHERES = 3
LMAX = 8
NX = 32
NY = 64
NZ = 512
NBX = 2
NBY = 4
NBZ = 32
COL_PTS = 256
RUNS = 8
TOTAL_PTS = 6144


def draw_point_ids(key, part):
    columns = NBX * NBY
    half = PB // 2
    keys = jax.random.split(key, SPHERES * columns)
    orders = jax.vmap(lambda subkey: jax.random.permutation(subkey, COL_PTS))(keys).reshape(SPHERES, columns, COL_PTS)
    base = (jnp.arange(SPHERES) * PTS)[:, None, None] + (jnp.arange(columns) * COL_PTS)[None, :, None]
    listed = (base + orders).astype(jnp.int32).reshape(SPHERES, columns, RUNS, half)
    layer = jnp.arange(RUNS + 1)
    earlier = listed[:, :, jnp.maximum(layer - 1, 0)]
    current = listed[:, :, jnp.minimum(layer, RUNS - 1)]
    live = ((layer >= 1) & (layer <= RUNS - 1))[None, None, :, None]
    current = jnp.where(live, current, TOTAL_PTS)
    lists = jnp.concatenate([earlier, current], 3).astype(jnp.int32)
    result = jnp.full((columns, NBZ, PB), TOTAL_PTS, jnp.int32)
    spacing = NBZ // SPHERES
    for sphere in range(SPHERES):
        result = result.at[:, sphere * spacing:sphere * spacing + RUNS + 1].set(lists[sphere])
    return result.reshape(NBX, NBY, NBZ, PB).astype(jnp.int32)


def levels(stream_key, shape, pieces, low, high):
    factor_of, own = 1.0, jax.random.fold_in(stream_key, 6)
    for dim, shards_of in pieces:
        heights = jnp.exp(jax.random.uniform(jax.random.fold_in(own, dim), (shards_of,), jnp.float32, low / len(pieces), high / len(pieces)))
        factor_of = factor_of * jnp.repeat(heights, shape[dim] // shards_of).reshape([-1 if axis == dim else 1 for axis in range(len(shape))])
    return factor_of


def normal_values(own_key, shape, scale, reach, pieces=(), held_as=jnp.bfloat16):
    values = scale * jax.random.normal(own_key, shape, jnp.float32)
    if pieces:
        values = values * levels(own_key, shape, pieces, -0.22, 0.18)
    return jnp.clip(values, -reach, reach).astype(held_as)


def setup_inputs(seed: int = 0) -> dict:
    key_list = jax.random.split(jax.random.key(seed), 7)
    return {
        "metric_pert": normal_values(key_list[0], (6, NX, NY, NZ), 0.3, 1.8, ((1, 2), (2, 4), (3, 4)), jnp.float32),
        "curvature": normal_values(key_list[1], (6, NX, NY, NZ), 1.0, 6.0, ((1, 2), (2, 4), (3, 4)), jnp.float32),
        "interp_weights": normal_values(key_list[2], (NBX, NBY, NBZ, PB, BLK * BLK * BLK), (BLK * BLK * BLK) ** -0.5, 0.09375, ((0, 2), (1, 4), (2, 4))),
        "point_ids": draw_point_ids(jax.random.fold_in(key_list[6], 71), 0),
        "theta": jnp.clip(jax.random.uniform(key_list[4], (TOTAL_PTS,), jnp.float32, 0.05, 3.09), 0.05, 3.09),
        "phi": jnp.clip(jax.random.uniform(key_list[5], (TOTAL_PTS,), jnp.float32, -3.140625, 3.140625), -3.140625, 3.140625),
    }


PAIRS = [[0, 1, 2], [1, 3, 4], [2, 4, 5]]

def build_table(degree_max):
    width = 2 * degree_max + 1
    columns = []
    orders = []
    for degree in range(2, degree_max + 1):
        for order in range(-degree, degree + 1):
            column = np.zeros(width * width)
            lead = (-1.0) ** order * math.sqrt(math.factorial(degree + order) * math.factorial(degree - order) * (2 * degree + 1) / (4.0 * math.pi * math.factorial(degree - 2) * math.factorial(degree + 2)))
            for step in range(0, degree + 3):
                lower = step - 2 - order
                if lower >= 0 and lower <= degree - 2:
                    value = lead * math.comb(degree + 2, step) * math.comb(degree - 2, lower) * (-1.0) ** (degree - step + 2)
                    expo = 2 * step - 2 - order
                    column[expo * width + (2 * degree - expo)] += value
            columns.append(column)
            orders.append(order)
    return (np.stack(columns, 1), np.array(orders))

def project(sphere_vals, theta, phi, member):
    table, orders = build_table(LMAX)
    width = 2 * LMAX + 1
    cosine = jnp.cos(theta * 0.5)
    sine = jnp.sin(theta * 0.5)
    cos_pow = jnp.stack([cosine ** power for power in range(width)], 1)
    sin_pow = jnp.stack([sine ** power for power in range(width)], 1)
    grid_pow = (cos_pow[:, :, None] * sin_pow[:, None, :]).reshape(theta.shape[0], width * width)
    amplitude = jnp.dot(grid_pow, jnp.asarray(table, jnp.float32), precision=lax.Precision.HIGHEST)
    angle_m = phi[:, None] * jnp.asarray(orders, jnp.float32)[None, :]
    y_real = amplitude * jnp.cos(angle_m)
    y_imag = amplitude * jnp.sin(angle_m)
    left_re = member * sphere_vals[0][None, :]
    left_im = member * sphere_vals[1][None, :]
    highest = lax.Precision.HIGHEST
    real = jnp.dot(left_re, y_real, precision=highest) + jnp.dot(left_im, y_imag, precision=highest)
    imag = jnp.dot(left_im, y_real, precision=highest) - jnp.dot(left_re, y_imag, precision=highest)
    return jnp.stack([real, imag], 1) * (4.0 * math.pi / PTS)

def weyl_scalar(padded, x_coord, y_coord, z_coord):
    extent = [x_coord.shape[0], y_coord.shape[0], z_coord.shape[0]]

    def moved(comp, axis, offset):
        index = [slice(2, 2 + count) for count in extent]
        index[axis] = slice(2 + offset, 2 + offset + extent[axis])
        return padded[comp][tuple(index)]

    def first(comp, axis):
        return (moved(comp, axis, -2) - 8.0 * moved(comp, axis, -1) + 8.0 * moved(comp, axis, 1) - moved(comp, axis, 2)) / 12.0

    def second(comp, axis):
        return (-moved(comp, axis, -2) + 16.0 * moved(comp, axis, -1) - 30.0 * moved(comp, axis, 0) + 16.0 * moved(comp, axis, 1) - moved(comp, axis, 2)) / 12.0
    kval = [moved(6 + comp, 0, 0) for comp in range(6)]
    trace = kval[0] + kval[3] + kval[5]
    electric = {}
    for row in range(3):
        for col in range(row, 3):
            comp = PAIRS[row][col]
            laplace = second(comp, 0) + second(comp, 1) + second(comp, 2)
            square = kval[PAIRS[row][0]] * kval[PAIRS[0][col]] + kval[PAIRS[row][1]] * kval[PAIRS[1][col]] + kval[PAIRS[row][2]] * kval[PAIRS[2][col]]
            value = -0.5 * laplace + trace * kval[comp] - square
            electric[row, col] = value
            electric[col, row] = value
    deriv = [[first(6 + comp, axis) for comp in range(6)] for axis in range(3)]
    curl = {}
    for row in range(3):
        one = (row + 1) % 3
        two = (row + 2) % 3
        for col in range(3):
            curl[row, col] = deriv[one][PAIRS[two][col]] - deriv[two][PAIRS[one][col]]
    x_full = x_coord[:, None, None]
    y_full = y_coord[None, :, None]
    z_full = z_coord[None, None, :]
    radial_xy = jnp.sqrt(x_full * x_full + y_full * y_full)
    radius = jnp.sqrt(radial_xy * radial_xy + z_full * z_full)
    cos_phi = x_full / radial_xy
    sin_phi = y_full / radial_xy
    cos_theta = z_full / radius
    sin_theta = radial_xy / radius
    e_theta = [cos_theta * cos_phi, cos_theta * sin_phi, -sin_theta]
    e_phi = [-sin_phi, cos_phi, 0.0 * cos_phi]
    real = 0.0
    imag = 0.0
    for row in range(3):
        for col in range(3):
            magnetic = 0.5 * (curl[row, col] + curl[col, row])
            plus = 0.5 * (e_theta[row] * e_theta[col] - e_phi[row] * e_phi[col])
            cross = 0.5 * (e_theta[row] * e_phi[col] + e_phi[row] * e_theta[col])
            real = real + electric[row, col] * plus - magnetic * cross
            imag = imag - electric[row, col] * cross - magnetic * plus
    return jnp.stack([real, imag]).astype(jnp.float32)

def reference(metric_pert, curvature, interp_weights, point_ids, theta, phi):
    fields = jnp.concatenate([metric_pert, curvature], 0)
    padded = jnp.pad(fields, ((0, 0), (2, 2), (2, 2), (2, 2)))
    size_x, size_y, size_z = (metric_pert.shape[1], metric_pert.shape[2], metric_pert.shape[3])
    y_coord = jnp.arange(size_y).astype(jnp.float32) + 0.5 - size_y / 2.0
    z_coord = jnp.arange(size_z).astype(jnp.float32) + 0.5 - size_z / 2.0
    slabs = []
    dense = jnp.zeros((TOTAL_PTS + 1, 2), jnp.float32)
    for block_x in range(NBX):
        slab = padded[:, block_x * BLK:block_x * BLK + BLK + 4]
        x_coord = (jnp.arange(BLK) + block_x * BLK).astype(jnp.float32) + 0.5 - size_x / 2.0
        psi_slab = weyl_scalar(slab, x_coord, y_coord, z_coord).astype(jnp.bfloat16)
        slabs.append(psi_slab)
        blocks = psi_slab.reshape(2, BLK, NBY, BLK, NBZ, BLK).transpose(2, 4, 0, 1, 3, 5).reshape(NBY, NBZ, 2, BLK * BLK * BLK)
        partial_value = jnp.einsum('yzcn,yzpn->yzpc', blocks.astype(jnp.float32), interp_weights[block_x].astype(jnp.float32), precision=lax.Precision.HIGHEST)
        dense = dense + jax.ops.segment_sum(partial_value.reshape(-1, 2), point_ids[block_x].reshape(-1), num_segments=TOTAL_PTS + 1)
    psi4_field = jnp.concatenate(slabs, 1)
    sphere_vals = dense[:TOTAL_PTS].T
    point_index = jnp.arange(TOTAL_PTS)
    member = (point_index[None, :] // PTS == jnp.arange(SPHERES)[:, None]).astype(jnp.float32)
    modes = project(sphere_vals, theta, phi, member)
    return (psi4_field, modes)
```

```python
import functools
import math

import jax
import jax.numpy as jnp
import numpy as np
from jax import lax
from jax.experimental import pallas as pl
from jax.experimental.pallas import tpu as pltpu
from jax.sharding import PartitionSpec as P

BLK = 16
PB = 64
PTS = 2048
SPHERES = 3
LMAX = 8
MODES = (LMAX + 1) ** 2 - 4
ROWS = -(-MODES // 8) * 8
WAVES = -(-(2 * LMAX + 1) // 16) * 16
AXES = ("gx", "gy", "gz")
MESH = pl.DeviceIdType.MESH
LOGICAL = pl.DeviceIdType.LOGICAL
LO = 8
PITCH = 24
DIRECT = 64
HELD = 4


def build_table():
    amplitude = np.zeros((ROWS, WAVES))
    pick_re = np.zeros((ROWS, WAVES))
    pick_im = np.zeros((ROWS, WAVES))
    for degree in range(2, LMAX + 1):
        base = degree * degree - 4
        for order in range(-degree, degree + 1):
            row = base + order + degree
            lead = (-1.0) ** order * math.sqrt(
                math.factorial(degree + order)
                * math.factorial(degree - order)
                * (2 * degree + 1)
                / (4.0 * math.pi * math.factorial(degree - 2) * math.factorial(degree + 2))
            )
            for step in range(0, degree + 3):
                lower = step - 2 - order
                if 0 <= lower <= degree - 2:
                    scale = (
                        lead
                        * math.comb(degree + 2, step)
                        * math.comb(degree - 2, lower)
                        * (-1.0) ** (degree - step + 2)
                    )
                    up, down = 2 * step - 2 - order, 2 * degree - 2 * step + 2 + order
                    wave = [1.0 + 0.0j]
                    for one, two in [(0.5, 0.5)] * up + [(-0.5j, 0.5j)] * down:
                        longer = [0.0j] * (len(wave) + 1)
                        for place, value in enumerate(wave):
                            longer[place + 1] += value * one
                            longer[place] += value * two
                        wave = longer
                    for j in range(degree + 1):
                        high, low = wave[degree + j], wave[degree - j]
                        amplitude[row, j] += scale * ((high + low).real if j else high.real)
                        if j:
                            amplitude[row, LMAX + j] += scale * (1j * (high - low)).real
            size = abs(order)
            pick_re[row, size] = 1.0
            if size:
                pick_im[row, LMAX + size] = 1.0 if order > 0 else -1.0
    table = np.concatenate([amplitude, pick_re, pick_im], 0).astype(np.float32)
    pieces = []
    for _ in range(3):
        pieces.append(table.astype(jnp.bfloat16))
        table = table - pieces[-1].astype(np.float32)
    return np.concatenate([pieces[n] for n in (0, 0, 1, 0, 1, 2)], 1)


def split(value, count):
    pieces = []
    for _ in range(count - 1):
        pieces.append(value.astype(jnp.bfloat16))
        value = value - pieces[-1].astype(jnp.float32)
    return pieces + [value.astype(jnp.bfloat16)]


def waves(gz, spacing, ids, theta_ref, phi_ref, wave_ref):
    blocks, slots = ids.shape
    per = PTS // 128
    wide = jnp.concatenate([ids] * (128 // slots), 1)
    low = lax.div(gz * blocks, spacing)
    high = jnp.minimum(low + 1, SPHERES - 1)
    layer = gz * blocks + lax.broadcasted_iota(jnp.int32, wide.shape, 0)
    later = layer >= (low + 1) * spacing
    point = wide - jnp.where(later, low + 1, low) * PTS
    row, lane = point >> 7, point & 127
    first = lax.broadcasted_iota(jnp.int32, wide.shape, 1) < slots
    angle = jnp.zeros(wide.shape, jnp.float32)

    def look_up(ref, index):
        one = jnp.broadcast_to(ref[pl.ds(low * per + index, 1), :], wide.shape)
        two = jnp.broadcast_to(ref[pl.ds(high * per + index, 1), :], wide.shape)
        return jnp.take_along_axis(jnp.where(later, two, one), lane, axis=1)

    for index in range(per):
        found = jnp.where(first, look_up(theta_ref, index), look_up(phi_ref, index))
        angle = jnp.where(row == index, found, angle)
    re, im = [jnp.ones(wide.shape, jnp.float32), jnp.cos(angle)], [None, jnp.sin(angle)]
    for j in range(2, LMAX + 1):
        a, b = j // 2, j - j // 2
        re.append(re[a] * re[b] - im[a] * im[b])
        im.append(re[a] * im[b] + im[a] * re[b])
    rows = re + im[1:]
    rows += [jnp.zeros(wide.shape, jnp.float32)] * (WAVES - len(rows))
    for place, value in enumerate(rows):
        wave_ref[place * blocks : (place + 1) * blocks, :] = value
    lane = lax.broadcasted_iota(jnp.int32, (8, 128), 1)
    result = [[], []]
    for pair in range(0, blocks, 2):
        columns = [[], []]
        for group in range(WAVES // 8):
            one = wave_ref[pl.ds(group * 8 * blocks + pair, 8, blocks), :]
            two = wave_ref[pl.ds(group * 8 * blocks + pair + 1, 8, blocks), :]
            columns[0].append(jnp.where(lane < slots, one, pltpu.roll(two, slots, 1)))
            columns[1].append(jnp.where(lane < slots, pltpu.roll(one, slots, 1), two))
        for side in range(2):
            result[side].append(jnp.concatenate(columns[side], 0))
    return tuple(jnp.concatenate(parts, 1) for parts in result)


def harmonics(in_theta, in_phi, table):
    def expand(rows, value):
        one, two, three = split(value, 3)
        stack = jnp.concatenate([one, two, one, three, two, one], 0)
        return jnp.dot(rows, stack, preferred_element_type=jnp.float32)

    amplitude = expand(table[:ROWS], in_theta)
    picked = expand(table[ROWS:], in_phi)
    re, im = split(amplitude * picked[:ROWS], 2), split(amplitude * picked[ROWS:], 2)
    return [jnp.concatenate([re[n], im[n]], 1) for n in range(2)]


def frame(x, y, z):
    rho2 = x * x + y * y
    inv_rho = lax.rsqrt(rho2)
    inv_radius = lax.rsqrt(rho2 + z * z)
    c, s = x * inv_rho, y * inv_rho
    cos_theta, sin_theta = z * inv_radius, rho2 * inv_rho * inv_radius
    cc, ss, cs = c * c, s * s, c * s
    square = cos_theta * cos_theta
    down = sin_theta * (1.0 / 24.0)
    cross = cos_theta * down
    turn = cos_theta * (1.0 / 24.0)
    return (
        (square * ss - cc) * (0.5 / 24.0), sin_theta * sin_theta * (0.5 / 24.0),
        (square + 1.0) * cs * (1.0 / 24.0), -cross * c, -cross * s,
        turn * cs, turn * (cc - ss), s * down, -c * down,
    )


def contract(weights, electric, magnetic):
    p, q = weights[:5], (weights[5], None) + tuple(weights[6:])

    def dot(weight, values):
        total = None
        for one, two in zip(weight, values):
            if one is not None and two is not None:
                total = one * two if total is None else total + one * two
        return total

    return -dot(p, electric) - dot(q, magnetic), dot(q, electric) - dot(p, magnetic)


def twist(a, b, c):
    one, two = b - a, b - c
    both = one + two
    return both + both, (one + one - two) * 2.0


def face_tile(axis, weights, laplace, deriv):
    electric = [laplace(comp) for comp in (3, 5, 1, 2, 4)]
    if axis == 0:
        c = deriv(10) * 2.0
        magnetic = (-c, c, -deriv(8), deriv(7), deriv(0))
    elif axis == 1:
        a = deriv(8) * -2.0
        magnetic = (a, a + a, deriv(10), deriv(11), -deriv(7))
    else:
        b = deriv(7) * 2.0
        magnetic = (b + b, b, -deriv(9), -deriv(10), deriv(8))
    return contract(weights, electric, magnetic)


def weyl_tile(field, weights):
    def along(comp, axis, offset):
        if axis == 0:
            return field(comp, offset, 0)
        if axis == 1:
            return field(comp, 0, offset)
        value = field(comp, 0, 0)
        return pltpu.roll(value, (-offset) % value.shape[1], 1)

    def first(comp, axis):
        near = along(comp, axis, 1) - along(comp, axis, -1)
        return near * 8.0 - (along(comp, axis, 2) - along(comp, axis, -2))

    xx, xy, xz, yy, yz, over = [field(6 + comp, 0, 0) for comp in range(6)]
    zz = over + xx
    part = yy - xx
    last = part.shape[1]
    yz2 = yz * yz
    square = (
        yz2 - xz * xz - part * zz,
        yz2 - xy * xy - yy * over,
        xz * yz - xy * zz,
        xy * yz - xz * yy,
        xy * xz - xx * yz,
    )
    electric = []
    for comp, value in zip((3, 5, 1, 2, 4), square):
        near, far = None, None
        for axis in range(3):
            one = along(comp, axis, 1) + along(comp, axis, -1)
            two = along(comp, axis, 2) + along(comp, axis, -2)
            near, far = (one, two) if near is None else (near + one, far + two)
        electric.append(value * 24.0 + near * 16.0 - far - field(comp, 0, 0) * 90.0)
    part_z = (pltpu.roll(part, last - 1, 1) - pltpu.roll(part, 1, 1)) * 8.0 - (
        pltpu.roll(part, last - 2, 1) - pltpu.roll(part, 2, 1)
    )
    magnetic = twist(first(8, 1), first(7, 2), first(10, 0)) + (
        first(10, 1) - part_z - first(8, 0),
        first(11, 1) - first(10, 2) + first(7, 0),
        first(8, 2) + first(0, 0) - first(7, 1),
    )
    return contract(weights, electric, magnetic)


def swap_blocks(tile):
    count = tile.shape[0]
    width = tile.shape[1] // count
    rolled = pltpu.roll(tile, 0, 1, stride=width, stride_axis=0)
    row = lax.broadcasted_iota(jnp.int32, tile.shape, 0)
    block = lax.broadcasted_iota(jnp.int32, tile.shape, 1) // width
    mixed = jnp.take_along_axis(rolled, (block - row + count) % count, axis=0)
    out = mixed
    for bit in range(3):
        shift = (1 << bit) * width
        out = jnp.where((row >> bit) & 1 == 1, pltpu.roll(out, tile.shape[1] - shift, 1), out)
    return out


def kernel(
    counts, metric, curvature, weights, ids_hbm, theta_hbm, phi_hbm, table_hbm,
    psi_ref, modes_ref,
    F, W, ids_ref, theta_ref, phi_ref, table_ref, wave_ref, FRAME, EDGE, POLL, T,
    PS, XS, XR, YS, YR, ZS, ZR, RED, MINE,
    load_sem, xs_sem, xr_sem, ys_sem, yr_sem, zs_sem, zr_sem, ps_sem, pr_sem,
):
    cx, cy, cz = psi_ref.shape[1:]
    blocks = cz // BLK
    spacing = blocks * counts["gz"] // SPHERES
    here = {axis: lax.axis_index(axis) for axis in AXES}
    loads = [
        pltpu.make_async_copy(source, target, load_sem.at[place])
        for place, (source, target) in enumerate((
            (metric, F.at[pl.ds(0, 6), pl.ds(2, cx), pl.ds(LO, cy)]),
            (curvature, F.at[pl.ds(6, 6), pl.ds(2, cx), pl.ds(LO, cy)]),
            (ids_hbm, ids_ref),
            (theta_hbm, theta_ref),
            (phi_hbm, phi_ref),
            (table_hbm, table_ref),
            (weights, W),
        ))
    ]
    for copy in loads:
        copy.start()

    def group_of(axes):
        total, rank, own = 1, 0, 0
        stride = math.prod(counts.values())
        strides = {}
        for axis in AXES:
            stride //= counts[axis]
            strides[axis] = stride
            own = own + here[axis] * stride
        for axis in axes:
            total *= counts[axis]
            rank = rank * counts[axis] + here[axis]
        unit = strides[axes[-1]]

        def peer(step):
            other = lax.rem(rank + step, total)
            return own + (other - rank) * unit

        return rank, total, peer

    if math.prod(counts.values()) <= DIRECT:
        groups = (group_of(AXES),)
    else:
        groups = (group_of(("gx", "gy")), group_of(("gz",)))
    barrier = pltpu.get_barrier_semaphore()
    with jax.named_scope("signal"):
        for _, count, peer in groups:
            for step in range(1, count):
                pl.semaphore_signal(barrier, inc=1, device_id=peer(step), device_id_type=LOGICAL)

    def coordinate(axis, cells, index):
        return (here[axis] * cells + index).astype(jnp.float32) + (0.5 - counts[axis] * cells / 2.0)

    tile = (8, cz)
    sub = lax.broadcasted_iota(jnp.int32, tile, 0)
    lane = lax.broadcasted_iota(jnp.int32, tile, 1)
    z = coordinate("gz", cz, lane)
    spot_of = ((lane + 2) & (cz - 1)) >> 2
    place = (lane + 2) & 3

    def layers(cells):
        return (
            (0, 0, -2, None, 0), (0, 1, -1, 0, 1),
            (1, 0, cells, cells - 1, cells - 2), (1, 1, cells + 1, None, cells - 1),
        )

    with jax.named_scope("zero"):
        for edge in (0, cx + 2):
            F[:, edge : edge + 2, LO : LO + cy, :] = jnp.zeros((12, 2, cy, cz), jnp.float32)
        for edge in (LO - 8, LO + cy):
            F[:, 2 : 2 + cx, edge : edge + 8, :] = jnp.zeros((12, cx, 8, cz), jnp.float32)
    with jax.named_scope("frames"):
        @pl.loop(0, cx)
        def _(x_index):
            x = coordinate("gx", cx, jnp.full(tile, x_index, jnp.int32))
            for part in range(cy // 8):
                for n, value in enumerate(frame(x, coordinate("gy", cy, sub + 8 * part), z)):
                    FRAME[n, x_index, 8 * part : 8 * part + 8, :] = value

        for at, (side, layer, cell, _, _) in enumerate(layers(cx)):
            for part in range(cy // 8):
                x = coordinate("gx", cx, jnp.full(tile, cell, jnp.int32))
                for n, value in enumerate(frame(x, coordinate("gy", cy, sub + 8 * part), z)):
                    EDGE[n, at, 8 * part : 8 * part + 8, :] = value
        for at, (side, layer, cell, _, _) in enumerate(layers(cy)):
            for part in range(cx // 8):
                y = coordinate("gy", cy, jnp.full(tile, cell, jnp.int32))
                for n, value in enumerate(frame(coordinate("gx", cx, sub + 8 * part), y, z)):
                    EDGE[n, 4 + at, 8 * part : 8 * part + 8, :] = value
        x = coordinate("gx", cx, spot_of % cx)
        y = coordinate("gy", cy, (spot_of // cx) * 8 + sub)
        beyond = coordinate("gz", cz, jnp.where(place >= 2, place - 4, cz + place))
        within = coordinate("gz", cz, jnp.where(place >= 2, cz + place - 4, place))
        for n, value in enumerate(frame(x, y, beyond)):
            EDGE[n, 8, :8, :] = value
        for n, value in enumerate(frame(x, y, within)):
            EDGE[n, 8, 8:16, :] = value

    with jax.named_scope("wait_fields"):
        loads[0].wait()
        loads[1].wait()

    with jax.named_scope("prepare"):
        @pl.loop(0, cx)
        def _(x_index):
            for part in range(cy // 8):
                rows = slice(LO + 8 * part, LO + 8 * part + 8)
                at = 2 + x_index
                h_xx, k_xx, k_zz = F[0, at, rows, :], F[6, at, rows, :], F[11, at, rows, :]
                F[3, at, rows, :] = F[3, at, rows, :] - h_xx
                F[5, at, rows, :] = F[5, at, rows, :] - h_xx
                F[0, at, rows, :] = F[9, at, rows, :] - k_zz
                F[11, at, rows, :] = k_zz - k_xx

    def face(axis, at, part, sign, near, far):
        def laplace(comp):
            return -far(comp) if near is None else near(comp) * 16.0 - far(comp)

        def deriv(comp):
            value = -far(comp) if near is None else near(comp) * 8.0 - far(comp)
            return value * sign

        weight = tuple(EDGE[n, at, 8 * part : 8 * part + 8, :] for n in range(9))
        return face_tile(axis, weight, laplace, functools.lru_cache(None)(deriv))

    with jax.named_scope("faces_x"):
        for at, (side, layer, _, near, far) in enumerate(layers(cx)):
            for part in range(cy // 8):
                rows = slice(LO + 8 * part, LO + 8 * part + 8)
                load = lambda at, rows=rows: None if at is None else lambda comp: F[comp, 2 + at, rows, :]
                real, imag = face(0, at, part, 1.0 - 2.0 * side, load(near), load(far))
                XS[side, 0, layer, 8 * part : 8 * part + 8, :] = real
                XS[side, 1, layer, 8 * part : 8 * part + 8, :] = imag
    pitch = F.shape[2]
    flat = F.reshape(12 * F.shape[1] * pitch, cz)
    with jax.named_scope("faces_y"):
        for at, (side, layer, _, near, far) in enumerate(layers(cy)):
            for part in range(cx // 8):
                start = (2 + 8 * part) * pitch + LO
                load = lambda at, start=start: None if at is None else lambda comp: flat[
                    pl.ds(comp * F.shape[1] * pitch + start + at, 8, pitch), :
                ]
                real, imag = face(1, 4 + at, part, 1.0 - 2.0 * side, load(near), load(far))
                YS[side, 0, layer, 8 * part : 8 * part + 8, :] = real
                YS[side, 1, layer, 8 * part : 8 * part + 8, :] = imag

    with jax.named_scope("faces_z"):
        @functools.lru_cache(None)
        def z_edges(comp):
            packed = None
            for part in range(cy // 8):
                rows = slice(LO + 8 * part, LO + 8 * part + 8)
                for x in range(cx):
                    spot = part * cx + x
                    moved = F[comp, 2 + x, rows, :]
                    if comp == 9:
                        moved = moved - F[6, 2 + x, rows, :]
                    if spot:
                        moved = jnp.where(spot_of == spot, pltpu.roll(moved, 4 * spot, 1), packed)
                    packed = moved
            return packed

        @functools.lru_cache(None)
        def z_near(comp):
            edges = z_edges(comp)
            return jnp.where(
                place == 3, pltpu.roll(edges, 1, 1), jnp.where(place == 0, pltpu.roll(edges, cz - 1, 1), 0.0)
            )

        sign = jnp.where(place >= 2, 1.0, -1.0)
        real, imag = face(2, 8, 0, sign, z_near, z_edges)
        ZS[0] = real
        ZS[1] = imag
        real, imag = face(2, 8, 1, sign, z_near, z_edges)
        POLL[0] = real
        POLL[1] = imag

    with jax.named_scope("barrier"):
        pl.semaphore_wait(barrier, sum(count - 1 for _, count, _ in groups))

    moves = []
    for axis, send, recv, send_sem, recv_sem in (
        ("gx", XS, XR, xs_sem, xr_sem), ("gy", YS, YR, ys_sem, yr_sem), ("gz", ZS, ZR, zs_sem, zr_sem)
    ):
        for side, has, target in ((0, here[axis] > 0, -1), (1, here[axis] < counts[axis] - 1, 1)):
            move = pltpu.make_async_remote_copy(
                src_ref=send if axis == "gz" else send.at[side],
                dst_ref=recv.at[1 - side],
                send_sem=send_sem.at[side],
                recv_sem=recv_sem.at[1 - side],
                device_id={axis: here[axis] + target},
                device_id_type=MESH,
            )
            arrival = pltpu.make_async_remote_copy(
                src_ref=send if axis == "gz" else send.at[side],
                dst_ref=recv.at[side],
                send_sem=send_sem.at[side],
                recv_sem=recv_sem.at[side],
                device_id={axis: here[axis] + target},
                device_id_type=MESH,
            )
            moves.append((has, move, arrival, recv, side))

            @pl.when(has)
            def _(move=move):
                move.start()

    with jax.named_scope("stencil"):
        @pl.loop(0, cx, unroll=16)
        def _(x_index):
            for part in range(cy // 8):
                rows = 8 * part

                def field(comp, dx, dy, rows=rows):
                    return F[comp, x_index + 2 + dx, LO + rows + dy : LO + rows + dy + 8, :]

                weight = tuple(FRAME[n, x_index, rows : rows + 8, :] for n in range(9))
                real, imag = weyl_tile(field, weight)
                PS[0, x_index, rows : rows + 8, :] = real
                PS[1, x_index, rows : rows + 8, :] = imag

    with jax.named_scope("harmonics"):
        for copy in loads[2:6]:
            copy.wait()
        ids = ids_ref[...]
        y_high, y_low = harmonics(*waves(here["gz"], spacing, ids, theta_ref, phi_ref, wave_ref), table_ref[...])
        sphere = jnp.concatenate([ids[b : b + 1] for b in range(ids.shape[0])], 1) // PTS

    with jax.named_scope("wait_halo"):
        for has, move, arrival, recv, side in moves:
            @pl.when(has)
            def _(arrival=arrival):
                arrival.wait_recv()

            @pl.when(jnp.logical_not(has))
            def _(recv=recv, side=side):
                recv[side] = jnp.zeros(recv.shape[1:], jnp.float32)

    with jax.named_scope("add_faces"):
        for side in range(2):
            for layer in range(2):
                x_at, y_at = layer + side * (cx - 2), layer + side * (cy - 2)
                for c in range(2):
                    PS[c, x_at] = PS[c, x_at] + XR[side, c, layer]
                    PS[c, :, y_at, :] = PS[c, :, y_at, :] + YR[side, c, layer]
        z_extra = [
            jnp.where(
                place < 2, pltpu.roll(ZR[1, c] - POLL[c], cz - 2, 1), pltpu.roll(ZR[0, c] - POLL[c], 2, 1)
            )
            for c in range(2)
        ]
    with jax.named_scope("wait_w"):
        loads[6].wait()
    with jax.named_scope("swap"):
        rim = (lane < 2) | (lane >= cz - 2)
        width = BLK * BLK
        for x_index in range(cx):
            parts = [[], []]
            for part in range(cy // 8):
                rows = 8 * part
                for c in range(2):
                    spot = part * cx + x_index
                    extra = pltpu.roll(z_extra[c], cz - 4 * spot, 1) if spot else z_extra[c]
                    parts[c].append(PS[c, x_index, rows : rows + 8, :] + jnp.where(rim, extra, 0.0))
            for c in range(2):
                psi_ref[c, x_index] = jnp.concatenate(parts[c], 0).astype(jnp.bfloat16)
            for part in range(cy // 8):
                both = [swap_blocks(parts[c][part]) for c in range(2)]
                at = x_index * width + part * 8 * BLK
                T[:, at : at + 8 * BLK] = jnp.concatenate(both, 0).astype(jnp.bfloat16)
    across = (((1,), (1,)), ((), ()))
    with jax.named_scope("interp"):
        acc = lax.dot_general(T[...], W[...], across, preferred_element_type=jnp.float32)
    with jax.named_scope("project"):
        row = lax.broadcasted_iota(jnp.int32, acc.shape, 0)
        slot = lax.broadcasted_iota(jnp.int32, acc.shape, 1)
        acc = jnp.where(row % blocks == slot // PB, acc, 0.0)
        v_re = jnp.sum(acc[:blocks], axis=0, keepdims=True)
        v_im = jnp.sum(acc[blocks:], axis=0, keepdims=True)
        row = lax.broadcasted_iota(jnp.int32, (8, W.shape[0]), 0)
        member = (row >> 1) + lax.div(here["gz"] * blocks, spacing) == sphere
        even = (row & 1) == 0
        v_one = jnp.where(member, jnp.where(even, v_re, v_im), 0.0)
        v_two = jnp.where(member, jnp.where(even, v_im, -v_re), 0.0)
        both = jnp.concatenate([v_one, v_two], 1) * (4.0 * math.pi / PTS)
        rest = both - both.astype(jnp.bfloat16).astype(jnp.float32)
        both = jnp.concatenate([both, rest], 0).astype(jnp.bfloat16)
        one = lax.dot_general(both, y_high, across, preferred_element_type=jnp.float32)
        two = lax.dot_general(both, y_low, across, preferred_element_type=jnp.float32)
        local = one[:8] + one[8:] + (two[:8] + two[8:])
        value = jnp.concatenate([local[:HELD], jnp.zeros((HELD, 128 - ROWS), jnp.float32)], 1)

    base = 0
    sends = []
    for phase, (me, count, peer) in enumerate(groups):
        with jax.named_scope(f"reduce{phase}"):
            MINE[phase] = value
            copies = [
                pltpu.make_async_remote_copy(
                    src_ref=MINE.at[phase],
                    dst_ref=RED.at[base + me],
                    send_sem=ps_sem.at[phase],
                    recv_sem=pr_sem.at[phase],
                    device_id=peer(step),
                    device_id_type=LOGICAL,
                )
                for step in range(1, count)
            ]
            for copy in copies:
                copy.start()
            RED[base + me] = value
        everything = pltpu.make_async_remote_copy(
            src_ref=RED.at[pl.ds(base, count - 1)],
            dst_ref=RED.at[pl.ds(base, count - 1)],
            send_sem=ps_sem.at[phase],
            recv_sem=pr_sem.at[phase],
            device_id=peer(1),
            device_id_type=LOGICAL,
        )
        with jax.named_scope(f"gather{phase}"):
            everything.wait_recv()
            last = phase == len(groups) - 1
            sums = []
            for lot in range(counts["gz"] if last else 1):
                members = range(lot, count, counts["gz"]) if last else range(count)
                value = None
                for other in members:
                    value = RED[base + other] if value is None else value + RED[base + other]
                sums.append(value)
        sends.append(everything)
        base += count
    for s in range(SPHERES):
        total = None
        for lot in range(counts["gz"]):
            at = 2 * (s - lot * blocks // spacing)
            if 0 <= at < HELD:
                piece = sums[lot][at : at + 2, :MODES]
                total = piece if total is None else total + piece
        modes_ref[s] = total
    with jax.named_scope("tail"):
        for copy in sends:
            copy.wait_send()
        for has, move, _, _, _ in moves:
            @pl.when(has)
            def _(move=move):
                move.wait_send()


def store_kernel(psi_ref, modes_ref, psi_out, modes_out, sem):
    copies = [
        pltpu.make_async_copy(psi_ref, psi_out, sem.at[0]),
        pltpu.make_async_copy(modes_ref, modes_out, sem.at[1]),
    ]
    for copy in copies:
        copy.start()
    for copy in copies:
        copy.wait()


def shards(counts, metric_pert, curvature, interp_weights, point_ids, theta, phi):
    _, cx, cy, cz = metric_pert.shape
    blocks = interp_weights.shape[2]
    points = theta.shape[0]
    vmem = pl.BlockSpec(memory_space=pltpu.VMEM)
    anywhere = pl.BlockSpec(memory_space=pl.ANY)
    many = math.prod(counts.values())
    total = many if many <= DIRECT else counts["gx"] * counts["gy"] + counts["gz"]
    phases = 1 if many <= DIRECT else 2
    dma = pltpu.SemaphoreType.DMA
    f32 = jnp.float32
    table = build_table()
    psi, modes = pl.pallas_call(
        functools.partial(kernel, counts),
        out_shape=(
            pltpu.VMEM((2, cx, cy, cz), jnp.bfloat16),
            pltpu.VMEM((SPHERES, 2, MODES), f32),
        ),
        in_specs=[anywhere] * 7,
        out_specs=(vmem, vmem),
        scratch_shapes=[
            pltpu.VMEM((12, cx + 5, LO + cy + PITCH - 8, cz), f32),
            pltpu.VMEM((blocks * PB, BLK * BLK * BLK), jnp.bfloat16),
            pltpu.VMEM((blocks, PB), jnp.int32),
            pltpu.VMEM((points // 128, 128), f32),
            pltpu.VMEM((points // 128, 128), f32),
            pltpu.VMEM(table.shape, jnp.bfloat16),
            pltpu.VMEM((WAVES * blocks, 128), f32),
            pltpu.VMEM((9, cx, cy, cz), f32),
            pltpu.VMEM((9, 9, 16, cz), f32),
            pltpu.VMEM((2, 8, cz), f32),
            pltpu.VMEM((2 * blocks, BLK * BLK * BLK), jnp.bfloat16),
            pltpu.VMEM((2, cx, cy, cz), f32),
            pltpu.VMEM((2, 2, 2, cy, cz), f32),
            pltpu.VMEM((2, 2, 2, cy, cz), f32),
            pltpu.VMEM((2, 2, 2, cx, cz), f32),
            pltpu.VMEM((2, 2, 2, cx, cz), f32),
            pltpu.VMEM((2, 8, cz), f32),
            pltpu.VMEM((2, 2, 8, cz), f32),
            pltpu.VMEM((total, HELD, 128), f32),
            pltpu.VMEM((2, HELD, 128), f32),
            dma((7,)), dma((2,)), dma((2,)), dma((2,)), dma((2,)), dma((2,)), dma((2,)),
            dma((phases,)), dma((phases,)),
        ],
        compiler_params=pltpu.CompilerParams(
            collective_id=0, has_side_effects=True, vmem_limit_bytes=60 * 1024 * 1024
        ),
    )(
        metric_pert,
        curvature,
        interp_weights.reshape(blocks * PB, BLK * BLK * BLK),
        point_ids.reshape(blocks, PB),
        theta.reshape(points // 128, 128),
        phi.reshape(points // 128, 128),
        jnp.asarray(table),
    )
    return pl.pallas_call(
        store_kernel,
        out_shape=(
            jax.ShapeDtypeStruct(psi.shape, psi.dtype),
            jax.ShapeDtypeStruct(modes.shape, modes.dtype),
        ),
        in_specs=[vmem, vmem],
        out_specs=(anywhere, anywhere),
        scratch_shapes=[dma((2,))],
        compiler_params=pltpu.CompilerParams(vmem_limit_bytes=1024 * 1024),
    )(psi, modes)


def solution(mesh):
    in_specs = (
        P(None, "gx", "gy", "gz"),
        P(None, "gx", "gy", "gz"),
        P("gx", "gy", "gz", None, None),
        P("gx", "gy", "gz", None),
        P(),
        P(),
    )
    out_specs = (P(None, "gx", "gy", "gz"), P())
    counts = {axis: mesh.shape[axis] for axis in AXES}
    return jax.shard_map(
        functools.partial(shards, counts), mesh=mesh, in_specs=in_specs, out_specs=out_specs, check_vma=False
    )
```

```python
import functools
import math

import jax
import jax.numpy as jnp
import numpy as np
from jax import lax
from jax.experimental import pallas as pl
from jax.experimental.pallas import tpu as pltpu
from jax.sharding import PartitionSpec as P

BLK = 16
PB = 64
PTS = 2048
SPHERES = 3
LMAX = 8
MODES = (LMAX + 1) ** 2 - 4
ROWS = -(-MODES // 8) * 8
WAVES = -(-(2 * LMAX + 1) // 16) * 16
AXES = ("gx", "gy", "gz")
MESH = pl.DeviceIdType.MESH
LOGICAL = pl.DeviceIdType.LOGICAL
LO = 8
PITCH = 24
DIRECT = 64
HELD = 4


def build_table():
    amplitude = np.zeros((ROWS, WAVES))
    pick_re = np.zeros((ROWS, WAVES))
    pick_im = np.zeros((ROWS, WAVES))
    for degree in range(2, LMAX + 1):
        base = degree * degree - 4
        for order in range(-degree, degree + 1):
            row = base + order + degree
            lead = (-1.0) ** order * math.sqrt(
                math.factorial(degree + order)
                * math.factorial(degree - order)
                * (2 * degree + 1)
                / (4.0 * math.pi * math.factorial(degree - 2) * math.factorial(degree + 2))
            )
            for step in range(0, degree + 3):
                lower = step - 2 - order
                if 0 <= lower <= degree - 2:
                    scale = (
                        lead
                        * math.comb(degree + 2, step)
                        * math.comb(degree - 2, lower)
                        * (-1.0) ** (degree - step + 2)
                    )
                    up, down = 2 * step - 2 - order, 2 * degree - 2 * step + 2 + order
                    wave = [1.0 + 0.0j]
                    for one, two in [(0.5, 0.5)] * up + [(-0.5j, 0.5j)] * down:
                        longer = [0.0j] * (len(wave) + 1)
                        for place, value in enumerate(wave):
                            longer[place + 1] += value * one
                            longer[place] += value * two
                        wave = longer
                    for j in range(degree + 1):
                        high, low = wave[degree + j], wave[degree - j]
                        amplitude[row, j] += scale * ((high + low).real if j else high.real)
                        if j:
                            amplitude[row, LMAX + j] += scale * (1j * (high - low)).real
            size = abs(order)
            pick_re[row, size] = 1.0
            if size:
                pick_im[row, LMAX + size] = 1.0 if order > 0 else -1.0
    table = np.concatenate([amplitude, pick_re, pick_im], 0).astype(np.float32)
    pieces = []
    for _ in range(3):
        pieces.append(table.astype(jnp.bfloat16))
        table = table - pieces[-1].astype(np.float32)
    return np.concatenate([pieces[n] for n in (0, 0, 1, 0, 1, 2)], 1)


def split(value, count):
    pieces = []
    for _ in range(count - 1):
        pieces.append(value.astype(jnp.bfloat16))
        value = value - pieces[-1].astype(jnp.float32)
    return pieces + [value.astype(jnp.bfloat16)]


def waves(gz, spacing, ids, theta_ref, phi_ref, wave_ref):
    blocks, slots = ids.shape
    per = PTS // 128
    wide = jnp.concatenate([ids] * (128 // slots), 1)
    low = lax.div(gz * blocks, spacing)
    high = jnp.minimum(low + 1, SPHERES - 1)
    layer = gz * blocks + lax.broadcasted_iota(jnp.int32, wide.shape, 0)
    later = layer >= (low + 1) * spacing
    point = wide - jnp.where(later, low + 1, low) * PTS
    row, lane = point >> 7, point & 127
    first = lax.broadcasted_iota(jnp.int32, wide.shape, 1) < slots
    angle = jnp.zeros(wide.shape, jnp.float32)

    def look_up(ref, index):
        one = jnp.broadcast_to(ref[pl.ds(low * per + index, 1), :], wide.shape)
        two = jnp.broadcast_to(ref[pl.ds(high * per + index, 1), :], wide.shape)
        return jnp.take_along_axis(jnp.where(later, two, one), lane, axis=1)

    for index in range(per):
        found = jnp.where(first, look_up(theta_ref, index), look_up(phi_ref, index))
        angle = jnp.where(row == index, found, angle)
    re, im = [jnp.ones(wide.shape, jnp.float32), jnp.cos(angle)], [None, jnp.sin(angle)]
    for j in range(2, LMAX + 1):
        a, b = j // 2, j - j // 2
        re.append(re[a] * re[b] - im[a] * im[b])
        im.append(re[a] * im[b] + im[a] * re[b])
    rows = re + im[1:]
    rows += [jnp.zeros(wide.shape, jnp.float32)] * (WAVES - len(rows))
    for place, value in enumerate(rows):
        wave_ref[place * blocks : (place + 1) * blocks, :] = value
    lane = lax.broadcasted_iota(jnp.int32, (8, 128), 1)
    result = [[], []]
    for pair in range(0, blocks, 2):
        columns = [[], []]
        for group in range(WAVES // 8):
            one = wave_ref[pl.ds(group * 8 * blocks + pair, 8, blocks), :]
            two = wave_ref[pl.ds(group * 8 * blocks + pair + 1, 8, blocks), :]
            columns[0].append(jnp.where(lane < slots, one, pltpu.roll(two, slots, 1)))
            columns[1].append(jnp.where(lane < slots, pltpu.roll(one, slots, 1), two))
        for side in range(2):
            result[side].append(jnp.concatenate(columns[side], 0))
    return tuple(jnp.concatenate(parts, 1) for parts in result)


def harmonics(in_theta, in_phi, table):
    def expand(rows, value):
        one, two, three = split(value, 3)
        stack = jnp.concatenate([one, two, one, three, two, one], 0)
        return jnp.dot(rows, stack, preferred_element_type=jnp.float32)

    amplitude = expand(table[:ROWS], in_theta)
    picked = expand(table[ROWS:], in_phi)
    re, im = split(amplitude * picked[:ROWS], 2), split(amplitude * picked[ROWS:], 2)
    return [jnp.concatenate([re[n], im[n]], 1) for n in range(2)]


def frame(x, y, z):
    rho2 = x * x + y * y
    inv_rho = lax.rsqrt(rho2)
    inv_radius = lax.rsqrt(rho2 + z * z)
    c, s = x * inv_rho, y * inv_rho
    cos_theta, sin_theta = z * inv_radius, rho2 * inv_rho * inv_radius
    cc, ss, cs = c * c, s * s, c * s
    square = cos_theta * cos_theta
    down = sin_theta * (1.0 / 24.0)
    cross = cos_theta * down
    turn = cos_theta * (1.0 / 24.0)
    return (
        (square * ss - cc) * (0.5 / 24.0), sin_theta * sin_theta * (0.5 / 24.0),
        (square + 1.0) * cs * (1.0 / 24.0), -cross * c, -cross * s,
        turn * cs, turn * (cc - ss), s * down, -c * down,
    )


def contract(weights, electric, magnetic):
    p, q = weights[:5], (weights[5], None) + tuple(weights[6:])

    def dot(weight, values):
        total = None
        for one, two in zip(weight, values):
            if one is not None and two is not None:
                total = one * two if total is None else total + one * two
        return total

    return -dot(p, electric) - dot(q, magnetic), dot(q, electric) - dot(p, magnetic)


def twist(a, b, c):
    one, two = b - a, b - c
    both = one + two
    return both + both, (one + one - two) * 2.0


def face_tile(axis, weights, laplace, deriv):
    electric = [laplace(comp) for comp in (3, 5, 1, 2, 4)]
    if axis == 0:
        c = deriv(10) * 2.0
        magnetic = (-c, c, -deriv(8), deriv(7), deriv(0))
    elif axis == 1:
        a = deriv(8) * -2.0
        magnetic = (a, a + a, deriv(10), deriv(11), -deriv(7))
    else:
        b = deriv(7) * 2.0
        magnetic = (b + b, b, -deriv(9), -deriv(10), deriv(8))
    return contract(weights, electric, magnetic)


def weyl_tile(field, weights):
    def along(comp, axis, offset):
        if axis == 0:
            return field(comp, offset, 0)
        if axis == 1:
            return field(comp, 0, offset)
        value = field(comp, 0, 0)
        return pltpu.roll(value, (-offset) % value.shape[1], 1)

    def first(comp, axis):
        near = along(comp, axis, 1) - along(comp, axis, -1)
        return near * 8.0 - (along(comp, axis, 2) - along(comp, axis, -2))

    xx, xy, xz, yy, yz, over = [field(6 + comp, 0, 0) for comp in range(6)]
    zz = over + xx
    part = yy - xx
    last = part.shape[1]
    yz2 = yz * yz
    square = (
        yz2 - xz * xz - part * zz,
        yz2 - xy * xy - yy * over,
        xz * yz - xy * zz,
        xy * yz - xz * yy,
        xy * xz - xx * yz,
    )
    electric = []
    for comp, value in zip((3, 5, 1, 2, 4), square):
        near, far = None, None
        for axis in range(3):
            one = along(comp, axis, 1) + along(comp, axis, -1)
            two = along(comp, axis, 2) + along(comp, axis, -2)
            near, far = (one, two) if near is None else (near + one, far + two)
        electric.append(value * 24.0 + near * 16.0 - far - field(comp, 0, 0) * 90.0)
    part_z = (pltpu.roll(part, last - 1, 1) - pltpu.roll(part, 1, 1)) * 8.0 - (
        pltpu.roll(part, last - 2, 1) - pltpu.roll(part, 2, 1)
    )
    magnetic = twist(first(8, 1), first(7, 2), first(10, 0)) + (
        first(10, 1) - part_z - first(8, 0),
        first(11, 1) - first(10, 2) + first(7, 0),
        first(8, 2) + first(0, 0) - first(7, 1),
    )
    return contract(weights, electric, magnetic)


def swap_blocks(tile):
    count = tile.shape[0]
    width = tile.shape[1] // count
    rolled = pltpu.roll(tile, 0, 1, stride=width, stride_axis=0)
    row = lax.broadcasted_iota(jnp.int32, tile.shape, 0)
    block = lax.broadcasted_iota(jnp.int32, tile.shape, 1) // width
    mixed = jnp.take_along_axis(rolled, (block + row + 1) % count, axis=0)
    return pltpu.roll(mixed, width, 1, stride=width, stride_axis=0)


def kernel(
    counts, metric, curvature, weights, ids_hbm, theta_hbm, phi_hbm, table_hbm,
    psi_ref, modes_ref,
    F, W, ids_ref, theta_ref, phi_ref, table_ref, wave_ref, FRAME, EDGE, POLL, T,
    PS, XS, XR, YS, YR, ZS, ZR, RED, MINE,
    load_sem, xs_sem, xr_sem, ys_sem, yr_sem, zs_sem, zr_sem, ps_sem, pr_sem,
):
    cx, cy, cz = psi_ref.shape[1:]
    blocks = cz // BLK
    spacing = blocks * counts["gz"] // SPHERES
    here = {axis: lax.axis_index(axis) for axis in AXES}
    loads = [
        pltpu.make_async_copy(source, target, load_sem.at[place])
        for place, (source, target) in enumerate((
            (metric, F.at[pl.ds(0, 6), pl.ds(2, cx), pl.ds(LO, cy)]),
            (curvature, F.at[pl.ds(6, 6), pl.ds(2, cx), pl.ds(LO, cy)]),
            (ids_hbm, ids_ref),
            (theta_hbm, theta_ref),
            (phi_hbm, phi_ref),
            (table_hbm, table_ref),
            (weights, W),
        ))
    ]
    for at in (2, 3, 4, 5, 0, 1):
        loads[at].start()

    def group_of(axes):
        total, rank, own = 1, 0, 0
        stride = math.prod(counts.values())
        strides = {}
        for axis in AXES:
            stride //= counts[axis]
            strides[axis] = stride
            own = own + here[axis] * stride
        for axis in axes:
            total *= counts[axis]
            rank = rank * counts[axis] + here[axis]
        unit = strides[axes[-1]]

        def target(other):
            return other if len(axes) == len(AXES) else own + (other - rank) * unit

        def peer(step):
            other = (rank + step) & (total - 1) if total & (total - 1) == 0 else lax.rem(rank + step, total)
            return target(other)

        def rising(step):
            return target(jnp.where(rank <= step - 1, step, step - 1))

        return rank, total, peer, rising

    if math.prod(counts.values()) <= DIRECT:
        groups = (group_of(AXES),)
    else:
        groups = (group_of(("gx", "gy")), group_of(("gz",)))
    barrier = pltpu.get_barrier_semaphore()
    with jax.named_scope("signal"):
        strides = [1, counts["gz"], counts["gy"] * counts["gz"]]
        for _, count, peer, _ in groups:
            near = [step for step in range(1, count) if min(step, count - step) in strides]
            for step in near + [step for step in range(1, count) if step not in near]:
                pl.semaphore_signal(barrier, inc=1, device_id=peer(step), device_id_type=LOGICAL)

    def coordinate(axis, cells, index):
        return (here[axis] * cells + index).astype(jnp.float32) + (0.5 - counts[axis] * cells / 2.0)

    tile = (8, cz)
    sub = lax.broadcasted_iota(jnp.int32, tile, 0)
    lane = lax.broadcasted_iota(jnp.int32, tile, 1)
    z = coordinate("gz", cz, lane)
    spot_of = ((lane + 2) & (cz - 1)) >> 2
    place = (lane + 2) & 3

    def layers(cells):
        return (
            (0, 0, -2, None, 0), (0, 1, -1, 0, 1),
            (1, 0, cells, cells - 1, cells - 2), (1, 1, cells + 1, None, cells - 1),
        )

    with jax.named_scope("zero"):
        for first, last in ((0, 6), (7, 9), (10, 12)):
            for edge in (0, cx + 2):
                F[first:last, edge : edge + 2, LO : LO + cy, :] = jnp.zeros((last - first, 2, cy, cz), jnp.float32)
            for edge in (LO - 8, LO + cy):
                F[first:last, 2 : 2 + cx, edge : edge + 8, :] = jnp.zeros((last - first, cx, 8, cz), jnp.float32)
    with jax.named_scope("frames"):
        @pl.loop(0, cx, unroll=4)
        def _(x_index):
            x = coordinate("gx", cx, jnp.full(tile, x_index, jnp.int32))
            for part in range(cy // 8):
                for n, value in enumerate(frame(x, coordinate("gy", cy, sub + 8 * part), z)):
                    FRAME[n, x_index, 8 * part : 8 * part + 8, :] = value

        for at, (side, layer, cell, _, _) in enumerate(layers(cx)):
            for part in range(cy // 8):
                x = coordinate("gx", cx, jnp.full(tile, cell, jnp.int32))
                for n, value in enumerate(frame(x, coordinate("gy", cy, sub + 8 * part), z)):
                    EDGE[n, at, 8 * part : 8 * part + 8, :] = value
        for at, (side, layer, cell, _, _) in enumerate(layers(cy)):
            for part in range(cx // 8):
                y = coordinate("gy", cy, jnp.full(tile, cell, jnp.int32))
                for n, value in enumerate(frame(coordinate("gx", cx, sub + 8 * part), y, z)):
                    EDGE[n, 4 + at, 8 * part : 8 * part + 8, :] = value
        x = coordinate("gx", cx, spot_of % cx)
        y = coordinate("gy", cy, (spot_of // cx) * 8 + sub)
        beyond = coordinate("gz", cz, jnp.where(place >= 2, place - 4, cz + place))
        within = coordinate("gz", cz, jnp.where(place >= 2, cz + place - 4, place))
        for n, value in enumerate(frame(x, y, beyond)):
            EDGE[n, 8, :8, :] = value
        for n, value in enumerate(frame(x, y, within)):
            EDGE[n, 8, 8:16, :] = value

    with jax.named_scope("harmonics"):
        for copy in loads[2:6]:
            copy.wait()
        ids = ids_ref[...]
        y_high, y_low = harmonics(*waves(here["gz"], spacing, ids, theta_ref, phi_ref, wave_ref), table_ref[...])
        sphere = jnp.concatenate([ids[b : b + 1] for b in range(ids.shape[0])], 1) // PTS

    with jax.named_scope("wait_fields"):
        loads[0].wait()
        loads[1].wait()
        loads[6].start()

    with jax.named_scope("prepare"):
        @pl.loop(0, cx)
        def _(x_index):
            for part in range(cy // 8):
                rows = slice(LO + 8 * part, LO + 8 * part + 8)
                at = 2 + x_index
                h_xx, k_xx, k_zz = F[0, at, rows, :], F[6, at, rows, :], F[11, at, rows, :]
                F[3, at, rows, :] = F[3, at, rows, :] - h_xx
                F[5, at, rows, :] = F[5, at, rows, :] - h_xx
                F[0, at, rows, :] = F[9, at, rows, :] - k_zz
                F[11, at, rows, :] = k_zz - k_xx

    def face(axis, at, part, sign, near, far):
        def laplace(comp):
            return -far(comp) if near is None else near(comp) * 16.0 - far(comp)

        def deriv(comp):
            value = -far(comp) if near is None else near(comp) * 8.0 - far(comp)
            return value * sign

        weight = tuple(EDGE[n, at, 8 * part : 8 * part + 8, :] for n in range(9))
        return face_tile(axis, weight, laplace, functools.lru_cache(None)(deriv))

    moves = []

    def exchange(axis, send, recv, send_sem, recv_sem):
        for side, has, target in ((0, here[axis] > 0, -1), (1, here[axis] < counts[axis] - 1, 1)):
            move = pltpu.make_async_remote_copy(
                src_ref=send if axis == "gz" else send.at[side],
                dst_ref=recv.at[1 - side],
                send_sem=send_sem.at[side],
                recv_sem=recv_sem.at[1 - side],
                device_id={axis: here[axis] + target},
                device_id_type=MESH,
            )
            arrival = pltpu.make_async_remote_copy(
                src_ref=send if axis == "gz" else send.at[side],
                dst_ref=recv.at[side],
                send_sem=send_sem.at[side],
                recv_sem=recv_sem.at[side],
                device_id={axis: here[axis] + target},
                device_id_type=MESH,
            )
            moves.append((has, move, arrival, recv, side))

            @pl.when(has)
            def _(move=move):
                move.start()

    with jax.named_scope("faces_x"):
        for at, (side, layer, _, near, far) in enumerate(layers(cx)):
            for part in range(cy // 8):
                rows = slice(LO + 8 * part, LO + 8 * part + 8)
                load = lambda at, rows=rows: None if at is None else lambda comp: F[comp, 2 + at, rows, :]
                real, imag = face(0, at, part, 1.0 - 2.0 * side, load(near), load(far))
                XS[side, 0, layer, 8 * part : 8 * part + 8, :] = real
                XS[side, 1, layer, 8 * part : 8 * part + 8, :] = imag
    with jax.named_scope("barrier"):
        pl.semaphore_wait(barrier, sum(group[1] - 1 for group in groups))
    exchange("gx", XS, XR, xs_sem, xr_sem)
    with jax.named_scope("faces_z"):
        packed = {}
        for part in range(cy // 8):
            rows = slice(LO + 8 * part, LO + 8 * part + 8)
            for x in range(cx):
                spot = part * cx + x
                mine = spot_of == spot
                for comp in (3, 5, 1, 2, 4, 7, 8, 9, 10):
                    moved = F[comp, 2 + x, rows, :]
                    if comp == 9:
                        moved = moved - F[6, 2 + x, rows, :]
                    if spot:
                        moved = jnp.where(mine, pltpu.roll(moved, 4 * spot, 1), packed[comp])
                    packed[comp] = moved
        z_edges = packed.__getitem__

        @functools.lru_cache(None)
        def z_near(comp):
            edges = z_edges(comp)
            return jnp.where(
                place == 3, pltpu.roll(edges, 1, 1), jnp.where(place == 0, pltpu.roll(edges, cz - 1, 1), 0.0)
            )

        sign = jnp.where(place >= 2, 1.0, -1.0)
        real, imag = face(2, 8, 0, sign, z_near, z_edges)
        ZS[0] = real
        ZS[1] = imag
        real, imag = face(2, 8, 1, sign, z_near, z_edges)
        POLL[0] = real
        POLL[1] = imag
    exchange("gz", ZS, ZR, zs_sem, zr_sem)
    pitch = F.shape[2]
    flat = F.reshape(12 * F.shape[1] * pitch, cz)
    with jax.named_scope("faces_y"):
        for at, (side, layer, _, near, far) in enumerate(layers(cy)):
            for part in range(cx // 8):
                start = (2 + 8 * part) * pitch + LO
                load = lambda at, start=start: None if at is None else lambda comp: flat[
                    pl.ds(comp * F.shape[1] * pitch + start + at, 8, pitch), :
                ]
                real, imag = face(1, 4 + at, part, 1.0 - 2.0 * side, load(near), load(far))
                YS[side, 0, layer, 8 * part : 8 * part + 8, :] = real
                YS[side, 1, layer, 8 * part : 8 * part + 8, :] = imag

    exchange("gy", YS, YR, ys_sem, yr_sem)

    with jax.named_scope("stencil"):
        @pl.loop(0, cx, unroll=16)
        def _(x_index):
            for part in range(cy // 8):
                rows = 8 * part

                def field(comp, dx, dy, rows=rows):
                    return F[comp, x_index + 2 + dx, LO + rows + dy : LO + rows + dy + 8, :]

                weight = tuple(FRAME[n, x_index, rows : rows + 8, :] for n in range(9))
                real, imag = weyl_tile(field, weight)
                PS[0, x_index, rows : rows + 8, :] = real
                PS[1, x_index, rows : rows + 8, :] = imag

    with jax.named_scope("wait_w"):
        loads[6].wait()
    with jax.named_scope("wait_halo"):
        for has, move, arrival, recv, side in moves:
            @pl.when(has)
            def _(arrival=arrival):
                arrival.wait_recv()

            @pl.when(jnp.logical_not(has))
            def _(recv=recv, side=side):
                recv[side] = jnp.zeros(recv.shape[1:], jnp.float32)

    spread = PS.reshape(2 * cx * cy, cz)
    with jax.named_scope("add_faces"):
        for side in range(2):
            for layer in range(2):
                x_at, y_at = layer + side * (cx - 2), layer + side * (cy - 2)
                for c in range(2):
                    PS[c, x_at] = PS[c, x_at] + XR[side, c, layer]
                    rows = pl.ds(c * cx * cy + y_at, cx, cy)
                    spread[rows, :] = spread[rows, :] + YR[side, c, layer]
        z_extra = [
            jnp.where(
                place < 2, pltpu.roll(ZR[1, c] - POLL[c], cz - 2, 1), pltpu.roll(ZR[0, c] - POLL[c], 2, 1)
            )
            for c in range(2)
        ]
    with jax.named_scope("swap"):
        rim = (lane < 2) | (lane >= cz - 2)
        width = BLK * BLK
        for x_index in range(cx):
            parts = [[], []]
            for part in range(cy // 8):
                rows = 8 * part
                for c in range(2):
                    spot = part * cx + x_index
                    extra = pltpu.roll(z_extra[c], cz - 4 * spot, 1) if spot else z_extra[c]
                    parts[c].append(PS[c, x_index, rows : rows + 8, :] + jnp.where(rim, extra, 0.0))
                    PS[c, x_index, rows : rows + 8, :] = parts[c][part]
            for part in range(cy // 8):
                both = [swap_blocks(parts[c][part]) for c in range(2)]
                at = x_index * width + part * 8 * BLK
                T[:, at : at + 8 * BLK] = jnp.concatenate(both, 0).astype(jnp.bfloat16)
    across = (((1,), (1,)), ((), ()))
    with jax.named_scope("interp"):
        acc = lax.dot_general(T[...], W[...], across, preferred_element_type=jnp.float32)
    with jax.named_scope("project"):
        row = lax.broadcasted_iota(jnp.int32, acc.shape, 0)
        slot = lax.broadcasted_iota(jnp.int32, acc.shape, 1)
        acc = jnp.where(blocks - 1 - row % blocks == slot // PB, acc, 0.0)
        v_re = jnp.sum(acc[:blocks], axis=0, keepdims=True)
        v_im = jnp.sum(acc[blocks:], axis=0, keepdims=True)
        row = lax.broadcasted_iota(jnp.int32, (8, W.shape[0]), 0)
        member = (row >> 1) + lax.div(here["gz"] * blocks, spacing) == sphere
        even = (row & 1) == 0
        v_one = jnp.where(member, jnp.where(even, v_re, v_im), 0.0)
        v_two = jnp.where(member, jnp.where(even, v_im, -v_re), 0.0)
        both = jnp.concatenate([v_one, v_two], 1) * (4.0 * math.pi / PTS)
        rest = both - both.astype(jnp.bfloat16).astype(jnp.float32)
        both = jnp.concatenate([both, rest], 0).astype(jnp.bfloat16)
        one = lax.dot_general(both, y_high, across, preferred_element_type=jnp.float32)
        two = lax.dot_general(both, y_low, across, preferred_element_type=jnp.float32)
        local = one[:8] + one[8:] + (two[:8] + two[8:])
        value = jnp.concatenate([local[:HELD], jnp.zeros((HELD, 128 - ROWS), jnp.float32)], 1)

    base = 0
    sends = []
    for phase, (me, count, peer, rising) in enumerate(groups):
        with jax.named_scope(f"reduce{phase}"):
            MINE[phase] = value
            copies = [
                pltpu.make_async_remote_copy(
                    src_ref=MINE.at[phase],
                    dst_ref=RED.at[base + me],
                    send_sem=ps_sem.at[phase],
                    recv_sem=pr_sem.at[phase],
                    device_id=rising(step),
                    device_id_type=LOGICAL,
                )
                for step in range(1, count)
            ]
            for copy in copies:
                copy.start()
            RED[base + me] = value
        everything = pltpu.make_async_remote_copy(
            src_ref=RED.at[pl.ds(base, count - 1)],
            dst_ref=RED.at[pl.ds(base, count - 1)],
            send_sem=ps_sem.at[phase],
            recv_sem=pr_sem.at[phase],
            device_id=peer(1),
            device_id_type=LOGICAL,
        )
        if phase == 0:
            with jax.named_scope("store_psi"):
                for c in range(2):
                    for x_index in range(cx):
                        psi_ref[c, x_index] = PS[c, x_index].astype(jnp.bfloat16)
        with jax.named_scope(f"gather{phase}"):
            everything.wait_recv()
            last = phase == len(groups) - 1
            sums = []
            for lot in range(counts["gz"] if last else 1):
                members = range(lot, count, counts["gz"]) if last else range(count)
                value = None
                for other in members:
                    value = RED[base + other] if value is None else value + RED[base + other]
                sums.append(value)
        sends.append(everything)
        base += count
    for s in range(SPHERES):
        total = None
        for lot in range(counts["gz"]):
            at = 2 * (s - lot * blocks // spacing)
            if 0 <= at < HELD:
                piece = sums[lot][at : at + 2, :MODES]
                total = piece if total is None else total + piece
        modes_ref[s] = total
    with jax.named_scope("tail"):
        for copy in sends:
            copy.wait_send()
        for has, move, _, _, _ in moves:
            @pl.when(has)
            def _(move=move):
                move.wait_send()


def store_kernel(psi_ref, modes_ref, psi_out, modes_out, sem):
    small = pltpu.make_async_copy(modes_ref, modes_out, sem.at[1])
    small.start()
    whole = pltpu.make_async_copy(psi_ref, psi_out, sem.at[0])
    for c in range(psi_ref.shape[0]):
        for half in range(2):
            rows = pl.ds(half * (psi_ref.shape[1] // 2), psi_ref.shape[1] // 2)
            pltpu.make_async_copy(psi_ref.at[c, rows], psi_out.at[c, rows], sem.at[0]).start()
    whole.wait()
    small.wait()


def shards(counts, metric_pert, curvature, interp_weights, point_ids, theta, phi):
    _, cx, cy, cz = metric_pert.shape
    blocks = interp_weights.shape[2]
    points = theta.shape[0]
    vmem = pl.BlockSpec(memory_space=pltpu.VMEM)
    anywhere = pl.BlockSpec(memory_space=pl.ANY)
    many = math.prod(counts.values())
    total = many if many <= DIRECT else counts["gx"] * counts["gy"] + counts["gz"]
    phases = 1 if many <= DIRECT else 2
    dma = pltpu.SemaphoreType.DMA
    f32 = jnp.float32
    table = build_table()
    psi, modes = pl.pallas_call(
        functools.partial(kernel, counts),
        out_shape=(
            pltpu.VMEM((2, cx, cy, cz), jnp.bfloat16),
            pltpu.VMEM((SPHERES, 2, MODES), f32),
        ),
        in_specs=[anywhere] * 7,
        out_specs=(vmem, vmem),
        scratch_shapes=[
            pltpu.VMEM((12, cx + 5, LO + cy + PITCH - 8, cz), f32),
            pltpu.VMEM((blocks * PB, BLK * BLK * BLK), jnp.bfloat16),
            pltpu.VMEM((blocks, PB), jnp.int32),
            pltpu.VMEM((points // 128, 128), f32),
            pltpu.VMEM((points // 128, 128), f32),
            pltpu.VMEM(table.shape, jnp.bfloat16),
            pltpu.VMEM((WAVES * blocks, 128), f32),
            pltpu.VMEM((9, cx, cy, cz), f32),
            pltpu.VMEM((9, 9, 16, cz), f32),
            pltpu.VMEM((2, 8, cz), f32),
            pltpu.VMEM((2 * blocks, BLK * BLK * BLK), jnp.bfloat16),
            pltpu.VMEM((2, cx, cy, cz), f32),
            pltpu.VMEM((2, 2, 2, cy, cz), f32),
            pltpu.VMEM((2, 2, 2, cy, cz), f32),
            pltpu.VMEM((2, 2, 2, cx, cz), f32),
            pltpu.VMEM((2, 2, 2, cx, cz), f32),
            pltpu.VMEM((2, 8, cz), f32),
            pltpu.VMEM((2, 2, 8, cz), f32),
            pltpu.VMEM((total, HELD, 128), f32),
            pltpu.VMEM((2, HELD, 128), f32),
            dma((7,)), dma((2,)), dma((2,)), dma((2,)), dma((2,)), dma((2,)), dma((2,)),
            dma((phases,)), dma((phases,)),
        ],
        compiler_params=pltpu.CompilerParams(
            collective_id=0, has_side_effects=True, vmem_limit_bytes=60 * 1024 * 1024
        ),
    )(
        metric_pert,
        curvature,
        interp_weights.reshape(blocks * PB, BLK * BLK * BLK),
        point_ids.reshape(blocks, PB),
        theta.reshape(points // 128, 128),
        phi.reshape(points // 128, 128),
        jnp.asarray(table),
    )
    return pl.pallas_call(
        store_kernel,
        out_shape=(
            jax.ShapeDtypeStruct(psi.shape, psi.dtype),
            jax.ShapeDtypeStruct(modes.shape, modes.dtype),
        ),
        in_specs=[vmem, vmem],
        out_specs=(anywhere, anywhere),
        scratch_shapes=[dma((2,))],
        compiler_params=pltpu.CompilerParams(vmem_limit_bytes=1024 * 1024),
    )(psi, modes)


def solution(mesh):
    in_specs = (
        P(None, "gx", "gy", "gz"),
        P(None, "gx", "gy", "gz"),
        P("gx", "gy", "gz", None, None),
        P("gx", "gy", "gz", None),
        P(),
        P(),
    )
    out_specs = (P(None, "gx", "gy", "gz"), P())
    counts = {axis: mesh.shape[axis] for axis in AXES}
    return jax.shard_map(
        functools.partial(shards, counts), mesh=mesh, in_specs=in_specs, out_specs=out_specs, check_vma=False
    )
```

```python
import functools
import math

import jax
import jax.numpy as jnp
import numpy as np
from jax import lax
from jax.experimental import pallas as pl
from jax.experimental.pallas import tpu as pltpu
from jax.sharding import PartitionSpec as P

BLK = 16
PB = 64
PTS = 2048
SPHERES = 3
LMAX = 8
MODES = (LMAX + 1) ** 2 - 4
ROWS = -(-MODES // 8) * 8
WAVES = -(-(2 * LMAX + 1) // 16) * 16
AXES = ("gx", "gy", "gz")
MESH = pl.DeviceIdType.MESH
LOGICAL = pl.DeviceIdType.LOGICAL
LO = 8
PITCH = 24
DIRECT = 64
HELD = 4


def build_table():
    amplitude = np.zeros((ROWS, WAVES))
    pick_re = np.zeros((ROWS, WAVES))
    pick_im = np.zeros((ROWS, WAVES))
    for degree in range(2, LMAX + 1):
        base = degree * degree - 4
        for order in range(-degree, degree + 1):
            row = base + order + degree
            lead = (-1.0) ** order * math.sqrt(
                math.factorial(degree + order)
                * math.factorial(degree - order)
                * (2 * degree + 1)
                / (4.0 * math.pi * math.factorial(degree - 2) * math.factorial(degree + 2))
            )
            for step in range(0, degree + 3):
                lower = step - 2 - order
                if 0 <= lower <= degree - 2:
                    scale = (
                        lead
                        * math.comb(degree + 2, step)
                        * math.comb(degree - 2, lower)
                        * (-1.0) ** (degree - step + 2)
                    )
                    up, down = 2 * step - 2 - order, 2 * degree - 2 * step + 2 + order
                    wave = [1.0 + 0.0j]
                    for one, two in [(0.5, 0.5)] * up + [(-0.5j, 0.5j)] * down:
                        longer = [0.0j] * (len(wave) + 1)
                        for place, value in enumerate(wave):
                            longer[place + 1] += value * one
                            longer[place] += value * two
                        wave = longer
                    for j in range(degree + 1):
                        high, low = wave[degree + j], wave[degree - j]
                        amplitude[row, j] += scale * ((high + low).real if j else high.real)
                        if j:
                            amplitude[row, LMAX + j] += scale * (1j * (high - low)).real
            size = abs(order)
            pick_re[row, size] = 1.0
            if size:
                pick_im[row, LMAX + size] = 1.0 if order > 0 else -1.0
    table = np.concatenate([amplitude, pick_re, pick_im], 0).astype(np.float32)
    pieces = []
    for _ in range(3):
        pieces.append(table.astype(jnp.bfloat16))
        table = table - pieces[-1].astype(np.float32)
    return np.concatenate([pieces[n] for n in (0, 0, 1, 0, 1, 2)], 1)


def split(value, count):
    pieces = []
    for _ in range(count - 1):
        pieces.append(value.astype(jnp.bfloat16))
        value = value - pieces[-1].astype(jnp.float32)
    return pieces + [value.astype(jnp.bfloat16)]


def waves(gz, spacing, ids, theta_ref, phi_ref, wave_ref):
    blocks, slots = ids.shape
    per = PTS // 128
    wide = jnp.concatenate([ids] * (128 // slots), 1)
    low = lax.div(gz * blocks, spacing)
    high = jnp.minimum(low + 1, SPHERES - 1)
    layer = gz * blocks + lax.broadcasted_iota(jnp.int32, wide.shape, 0)
    later = layer >= (low + 1) * spacing
    point = wide - jnp.where(later, low + 1, low) * PTS
    row, lane = point >> 7, point & 127
    first = lax.broadcasted_iota(jnp.int32, wide.shape, 1) < slots
    angle = jnp.zeros(wide.shape, jnp.float32)

    def look_up(ref, index):
        one = jnp.broadcast_to(ref[pl.ds(low * per + index, 1), :], wide.shape)
        two = jnp.broadcast_to(ref[pl.ds(high * per + index, 1), :], wide.shape)
        return jnp.take_along_axis(jnp.where(later, two, one), lane, axis=1)

    for index in range(per):
        found = jnp.where(first, look_up(theta_ref, index), look_up(phi_ref, index))
        angle = jnp.where(row == index, found, angle)
    re, im = [jnp.ones(wide.shape, jnp.float32), jnp.cos(angle)], [None, jnp.sin(angle)]
    for j in range(2, LMAX + 1):
        a, b = j // 2, j - j // 2
        re.append(re[a] * re[b] - im[a] * im[b])
        im.append(re[a] * im[b] + im[a] * re[b])
    rows = re + im[1:]
    rows += [jnp.zeros(wide.shape, jnp.float32)] * (WAVES - len(rows))
    for place, value in enumerate(rows):
        wave_ref[place * blocks : (place + 1) * blocks, :] = value
    lane = lax.broadcasted_iota(jnp.int32, (8, 128), 1)
    result = [[], []]
    for pair in range(0, blocks, 2):
        columns = [[], []]
        for group in range(WAVES // 8):
            one = wave_ref[pl.ds(group * 8 * blocks + pair, 8, blocks), :]
            two = wave_ref[pl.ds(group * 8 * blocks + pair + 1, 8, blocks), :]
            columns[0].append(jnp.where(lane < slots, one, pltpu.roll(two, slots, 1)))
            columns[1].append(jnp.where(lane < slots, pltpu.roll(one, slots, 1), two))
        for side in range(2):
            result[side].append(jnp.concatenate(columns[side], 0))
    return tuple(jnp.concatenate(parts, 1) for parts in result)


def harmonics(in_theta, in_phi, table):
    def expand(rows, value):
        one, two, three = split(value, 3)
        stack = jnp.concatenate([one, two, one, three, two, one], 0)
        return jnp.dot(rows, stack, preferred_element_type=jnp.float32)

    amplitude = expand(table[:ROWS], in_theta)
    picked = expand(table[ROWS:], in_phi)
    re, im = split(amplitude * picked[:ROWS], 2), split(amplitude * picked[ROWS:], 2)
    return [jnp.concatenate([re[n], im[n]], 1) for n in range(2)]


def frame(x, y, z):
    rho2 = x * x + y * y
    inv_rho = lax.rsqrt(rho2)
    inv_radius = lax.rsqrt(rho2 + z * z)
    c, s = x * inv_rho, y * inv_rho
    cos_theta, sin_theta = z * inv_radius, rho2 * inv_rho * inv_radius
    cc, ss, cs = c * c, s * s, c * s
    square = cos_theta * cos_theta
    down = sin_theta * (1.0 / 24.0)
    cross = cos_theta * down
    turn = cos_theta * (1.0 / 24.0)
    return (
        (square * ss - cc) * (0.5 / 24.0), sin_theta * sin_theta * (0.5 / 24.0),
        (square + 1.0) * cs * (1.0 / 24.0), -cross * c, -cross * s,
        turn * cs, turn * (cc - ss), s * down, -c * down,
    )


def contract(weights, electric, magnetic):
    p, q = weights[:5], (weights[5], None) + tuple(weights[6:])

    def dot(weight, values):
        total = None
        for one, two in zip(weight, values):
            if one is not None and two is not None:
                total = one * two if total is None else total + one * two
        return total

    return -dot(p, electric) - dot(q, magnetic), dot(q, electric) - dot(p, magnetic)


def twist(a, b, c):
    one, two = b - a, b - c
    both = one + two
    return both + both, (one + one - two) * 2.0


def face_tile(axis, weights, laplace, deriv):
    electric = [laplace(comp) for comp in (3, 5, 1, 2, 4)]
    if axis == 0:
        c = deriv(10) * 2.0
        magnetic = (-c, c, -deriv(8), deriv(7), deriv(0))
    elif axis == 1:
        a = deriv(8) * -2.0
        magnetic = (a, a + a, deriv(10), deriv(11), -deriv(7))
    else:
        b = deriv(7) * 2.0
        magnetic = (b + b, b, -deriv(9), -deriv(10), deriv(8))
    return contract(weights, electric, magnetic)


def weyl_tile(field, weights):
    def along(comp, axis, offset):
        if axis == 0:
            return field(comp, offset, 0)
        if axis == 1:
            return field(comp, 0, offset)
        value = field(comp, 0, 0)
        return pltpu.roll(value, (-offset) % value.shape[1], 1)

    def first(comp, axis):
        near = along(comp, axis, 1) - along(comp, axis, -1)
        return near * 8.0 - (along(comp, axis, 2) - along(comp, axis, -2))

    xx, xy, xz, yy, yz, over = [field(6 + comp, 0, 0) for comp in range(6)]
    zz = over + xx
    part = yy - xx
    last = part.shape[1]
    yz2 = yz * yz
    square = (
        yz2 - xz * xz - part * zz,
        yz2 - xy * xy - yy * over,
        xz * yz - xy * zz,
        xy * yz - xz * yy,
        xy * xz - xx * yz,
    )
    electric = []
    for comp, value in zip((3, 5, 1, 2, 4), square):
        near, far = None, None
        for axis in range(3):
            one = along(comp, axis, 1) + along(comp, axis, -1)
            two = along(comp, axis, 2) + along(comp, axis, -2)
            near, far = (one, two) if near is None else (near + one, far + two)
        electric.append(value * 24.0 + near * 16.0 - far - field(comp, 0, 0) * 90.0)
    part_z = (pltpu.roll(part, last - 1, 1) - pltpu.roll(part, 1, 1)) * 8.0 - (
        pltpu.roll(part, last - 2, 1) - pltpu.roll(part, 2, 1)
    )
    magnetic = twist(first(8, 1), first(7, 2), first(10, 0)) + (
        first(10, 1) - part_z - first(8, 0),
        first(11, 1) - first(10, 2) + first(7, 0),
        first(8, 2) + first(0, 0) - first(7, 1),
    )
    return contract(weights, electric, magnetic)


def swap_blocks(tile):
    count = tile.shape[0]
    width = tile.shape[1] // count
    rolled = pltpu.roll(tile, 0, 1, stride=width, stride_axis=0)
    row = lax.broadcasted_iota(jnp.int32, tile.shape, 0)
    block = lax.broadcasted_iota(jnp.int32, tile.shape, 1) // width
    mixed = jnp.take_along_axis(rolled, (block + row + 1) % count, axis=0)
    return pltpu.roll(mixed, width, 1, stride=width, stride_axis=0)


def kernel(
    counts, metric, curvature, weights, ids_hbm, theta_hbm, phi_hbm, table_hbm,
    psi_ref, modes_ref,
    F, W, ids_ref, theta_ref, phi_ref, table_ref, wave_ref, FRAME, EDGE, POLL, T,
    PS, XS, XR, YS, YR, ZS, ZR, RED, MINE,
    load_sem, xs_sem, xr_sem, ys_sem, yr_sem, zs_sem, zr_sem, ps_sem, pr_sem,
):
    cx, cy, cz = psi_ref.shape[1:]
    blocks = cz // BLK
    spacing = blocks * counts["gz"] // SPHERES
    here = {axis: lax.axis_index(axis) for axis in AXES}
    loads = [
        pltpu.make_async_copy(source, target, load_sem.at[max(place - 1, 0)])
        for place, (source, target) in enumerate((
            (metric, F.at[pl.ds(0, 6), pl.ds(2, cx), pl.ds(LO, cy)]),
            (curvature, F.at[pl.ds(6, 6), pl.ds(2, cx), pl.ds(LO, cy)]),
            (ids_hbm, ids_ref),
            (theta_hbm, theta_ref),
            (phi_hbm, phi_ref),
            (table_hbm, table_ref),
            (weights, W),
        ))
    ]
    for at in (2, 3, 4, 5, 0, 1):
        loads[at].start()

    def group_of(axes):
        total, rank, own = 1, 0, 0
        stride = math.prod(counts.values())
        strides = {}
        for axis in AXES:
            stride //= counts[axis]
            strides[axis] = stride
            own = own + here[axis] * stride
        for axis in axes:
            total *= counts[axis]
            rank = rank * counts[axis] + here[axis]
        unit = strides[axes[-1]]

        def target(other):
            return other if len(axes) == len(AXES) else own + (other - rank) * unit

        def peer(step):
            other = (rank + step) & (total - 1) if total & (total - 1) == 0 else lax.rem(rank + step, total)
            return target(other)

        def rising(step):
            return target(jnp.where(rank <= step - 1, step, step - 1))

        return rank, total, peer, rising

    if math.prod(counts.values()) <= DIRECT:
        groups = (group_of(AXES),)
    else:
        groups = (group_of(("gx", "gy")), group_of(("gz",)))
    barrier = pltpu.get_barrier_semaphore()
    with jax.named_scope("signal"):
        strides = [1, counts["gz"], counts["gy"] * counts["gz"]]
        for _, count, peer, _ in groups:
            near = [step for step in range(1, count) if min(step, count - step) in strides]
            for step in near + [step for step in range(1, count) if step not in near]:
                pl.semaphore_signal(barrier, inc=1, device_id=peer(step), device_id_type=LOGICAL)

    def coordinate(axis, cells, index):
        return (here[axis] * cells + index).astype(jnp.float32) + (0.5 - counts[axis] * cells / 2.0)

    tile = (8, cz)
    sub = lax.broadcasted_iota(jnp.int32, tile, 0)
    lane = lax.broadcasted_iota(jnp.int32, tile, 1)
    z = coordinate("gz", cz, lane)
    spot_of = ((lane + 2) & (cz - 1)) >> 2
    place = (lane + 2) & 3

    def layers(cells):
        return (
            (0, 0, -2, None, 0), (0, 1, -1, 0, 1),
            (1, 0, cells, cells - 1, cells - 2), (1, 1, cells + 1, None, cells - 1),
        )

    with jax.named_scope("zero"):
        for first, last in ((0, 6), (7, 9), (10, 12)):
            for edge in (0, cx + 2):
                F[first:last, edge : edge + 2, LO : LO + cy, :] = jnp.zeros((last - first, 2, cy, cz), jnp.float32)
            for edge in (LO - 8, LO + cy):
                F[first:last, 2 : 2 + cx, edge : edge + 8, :] = jnp.zeros((last - first, cx, 8, cz), jnp.float32)
    with jax.named_scope("frames"):
        @pl.loop(0, cx, unroll=4)
        def _(x_index):
            x = coordinate("gx", cx, jnp.full(tile, x_index, jnp.int32))
            for part in range(cy // 8):
                for n, value in enumerate(frame(x, coordinate("gy", cy, sub + 8 * part), z)):
                    FRAME[n, x_index, 8 * part : 8 * part + 8, :] = value

        for at, (side, layer, cell, _, _) in enumerate(layers(cx)):
            for part in range(cy // 8):
                x = coordinate("gx", cx, jnp.full(tile, cell, jnp.int32))
                for n, value in enumerate(frame(x, coordinate("gy", cy, sub + 8 * part), z)):
                    EDGE[n, at, 8 * part : 8 * part + 8, :] = value
        for at, (side, layer, cell, _, _) in enumerate(layers(cy)):
            for part in range(cx // 8):
                y = coordinate("gy", cy, jnp.full(tile, cell, jnp.int32))
                for n, value in enumerate(frame(coordinate("gx", cx, sub + 8 * part), y, z)):
                    EDGE[n, 4 + at, 8 * part : 8 * part + 8, :] = value
        x = coordinate("gx", cx, spot_of % cx)
        y = coordinate("gy", cy, (spot_of // cx) * 8 + sub)
        beyond = coordinate("gz", cz, jnp.where(place >= 2, place - 4, cz + place))
        within = coordinate("gz", cz, jnp.where(place >= 2, cz + place - 4, place))
        for n, value in enumerate(frame(x, y, beyond)):
            EDGE[n, 8, :8, :] = value
        for n, value in enumerate(frame(x, y, within)):
            EDGE[n, 8, 8:16, :] = value

    with jax.named_scope("harmonics"):
        for copy in loads[2:6]:
            copy.wait()
        ids = ids_ref[...]
        y_high, y_low = harmonics(*waves(here["gz"], spacing, ids, theta_ref, phi_ref, wave_ref), table_ref[...])
        sphere = jnp.concatenate([ids[b : b + 1] for b in range(ids.shape[0])], 1) // PTS

    with jax.named_scope("wait_fields"):
        cells = F.at[pl.ds(0, 12), pl.ds(2, cx), pl.ds(LO, cy)]
        pltpu.make_async_copy(cells, cells, load_sem.at[0]).wait()
        loads[6].start()

    with jax.named_scope("prepare"):
        @pl.loop(0, cx)
        def _(x_index):
            for part in range(cy // 8):
                rows = slice(LO + 8 * part, LO + 8 * part + 8)
                at = 2 + x_index
                h_xx, k_xx, k_zz = F[0, at, rows, :], F[6, at, rows, :], F[11, at, rows, :]
                F[3, at, rows, :] = F[3, at, rows, :] - h_xx
                F[5, at, rows, :] = F[5, at, rows, :] - h_xx
                F[0, at, rows, :] = F[9, at, rows, :] - k_zz
                F[11, at, rows, :] = k_zz - k_xx

    def face(axis, at, part, sign, near, far):
        def laplace(comp):
            return -far(comp) if near is None else near(comp) * 16.0 - far(comp)

        def deriv(comp):
            value = -far(comp) if near is None else near(comp) * 8.0 - far(comp)
            return value * sign

        weight = tuple(EDGE[n, at, 8 * part : 8 * part + 8, :] for n in range(9))
        return face_tile(axis, weight, laplace, functools.lru_cache(None)(deriv))

    moves, send_sems = [], []

    def exchange(axis, send, recv, send_sem, recv_sem):
        send_sems.append(send_sem)
        for side, has, target in ((0, here[axis] > 0, -1), (1, here[axis] < counts[axis] - 1, 1)):
            move = pltpu.make_async_remote_copy(
                src_ref=send if axis == "gz" else send.at[side],
                dst_ref=recv.at[1 - side],
                send_sem=send_sem.at[0],
                recv_sem=recv_sem.at[1 - side],
                device_id={axis: here[axis] + target},
                device_id_type=MESH,
            )
            arrival = pltpu.make_async_remote_copy(
                src_ref=send if axis == "gz" else send.at[side],
                dst_ref=recv.at[side],
                send_sem=send_sem.at[0],
                recv_sem=recv_sem.at[side],
                device_id={axis: here[axis] + target},
                device_id_type=MESH,
            )
            moves.append((has, move, arrival, recv, side))

            @pl.when(has)
            def _(move=move):
                move.start()

    with jax.named_scope("faces_x"):
        for at, (side, layer, _, near, far) in enumerate(layers(cx)):
            for part in range(cy // 8):
                rows = slice(LO + 8 * part, LO + 8 * part + 8)
                load = lambda at, rows=rows: None if at is None else lambda comp: F[comp, 2 + at, rows, :]
                real, imag = face(0, at, part, 1.0 - 2.0 * side, load(near), load(far))
                XS[side, 0, layer, 8 * part : 8 * part + 8, :] = real
                XS[side, 1, layer, 8 * part : 8 * part + 8, :] = imag
    with jax.named_scope("barrier"):
        pl.semaphore_wait(barrier, sum(group[1] - 1 for group in groups))
    exchange("gx", XS, XR, xs_sem, xr_sem)
    with jax.named_scope("faces_z"):
        packed = {}
        for part in range(cy // 8):
            rows = slice(LO + 8 * part, LO + 8 * part + 8)
            for x in range(cx):
                spot = part * cx + x
                mine = spot_of == spot
                for comp in (3, 5, 1, 2, 4, 7, 8, 9, 10):
                    moved = F[comp, 2 + x, rows, :]
                    if comp == 9:
                        moved = moved - F[6, 2 + x, rows, :]
                    if spot:
                        moved = jnp.where(mine, pltpu.roll(moved, 4 * spot, 1), packed[comp])
                    packed[comp] = moved
        z_edges = packed.__getitem__

        @functools.lru_cache(None)
        def z_near(comp):
            edges = z_edges(comp)
            return jnp.where(
                place == 3, pltpu.roll(edges, 1, 1), jnp.where(place == 0, pltpu.roll(edges, cz - 1, 1), 0.0)
            )

        sign = jnp.where(place >= 2, 1.0, -1.0)
        real, imag = face(2, 8, 0, sign, z_near, z_edges)
        ZS[0] = real
        ZS[1] = imag
        real, imag = face(2, 8, 1, sign, z_near, z_edges)
        POLL[0] = real
        POLL[1] = imag
    exchange("gz", ZS, ZR, zs_sem, zr_sem)
    pitch = F.shape[2]
    flat = F.reshape(12 * F.shape[1] * pitch, cz)
    with jax.named_scope("faces_y"):
        for at, (side, layer, _, near, far) in enumerate(layers(cy)):
            for part in range(cx // 8):
                start = (2 + 8 * part) * pitch + LO
                load = lambda at, start=start: None if at is None else lambda comp: flat[
                    pl.ds(comp * F.shape[1] * pitch + start + at, 8, pitch), :
                ]
                real, imag = face(1, 4 + at, part, 1.0 - 2.0 * side, load(near), load(far))
                YS[side, 0, layer, 8 * part : 8 * part + 8, :] = real
                YS[side, 1, layer, 8 * part : 8 * part + 8, :] = imag

    exchange("gy", YS, YR, ys_sem, yr_sem)

    with jax.named_scope("stencil"):
        @pl.loop(0, cx, unroll=16)
        def _(x_index):
            for part in range(cy // 8):
                rows = 8 * part

                def field(comp, dx, dy, rows=rows):
                    return F[comp, x_index + 2 + dx, LO + rows + dy : LO + rows + dy + 8, :]

                weight = tuple(FRAME[n, x_index, rows : rows + 8, :] for n in range(9))
                real, imag = weyl_tile(field, weight)
                PS[0, x_index, rows : rows + 8, :] = real
                PS[1, x_index, rows : rows + 8, :] = imag

    with jax.named_scope("wait_w"):
        loads[6].wait()
    with jax.named_scope("wait_halo"):
        for has, move, arrival, recv, side in moves:
            @pl.when(has)
            def _(arrival=arrival):
                arrival.wait_recv()

            @pl.when(jnp.logical_not(has))
            def _(recv=recv, side=side):
                recv[side] = jnp.zeros(recv.shape[1:], jnp.float32)

    spread = PS.reshape(2 * cx * cy, cz)
    with jax.named_scope("add_faces"):
        for side in range(2):
            for layer in range(2):
                x_at, y_at = layer + side * (cx - 2), layer + side * (cy - 2)
                for c in range(2):
                    PS[c, x_at] = PS[c, x_at] + XR[side, c, layer]
                    rows = pl.ds(c * cx * cy + y_at, cx, cy)
                    spread[rows, :] = spread[rows, :] + YR[side, c, layer]
        z_extra = [
            jnp.where(
                place < 2, pltpu.roll(ZR[1, c] - POLL[c], cz - 2, 1), pltpu.roll(ZR[0, c] - POLL[c], 2, 1)
            )
            for c in range(2)
        ]
    with jax.named_scope("swap"):
        rim = (lane < 2) | (lane >= cz - 2)
        width = BLK * BLK
        for x_index in range(cx):
            parts = [[], []]
            for part in range(cy // 8):
                rows = 8 * part
                for c in range(2):
                    spot = part * cx + x_index
                    extra = pltpu.roll(z_extra[c], cz - 4 * spot, 1) if spot else z_extra[c]
                    parts[c].append(PS[c, x_index, rows : rows + 8, :] + jnp.where(rim, extra, 0.0))
                    PS[c, x_index, rows : rows + 8, :] = parts[c][part]
            for part in range(cy // 8):
                both = [swap_blocks(parts[c][part]) for c in range(2)]
                at = x_index * width + part * 8 * BLK
                T[:, at : at + 8 * BLK] = jnp.concatenate(both, 0).astype(jnp.bfloat16)
    across = (((1,), (1,)), ((), ()))
    with jax.named_scope("interp"):
        acc = lax.dot_general(T[...], W[...], across, preferred_element_type=jnp.float32)
    with jax.named_scope("project"):
        row = lax.broadcasted_iota(jnp.int32, acc.shape, 0)
        slot = lax.broadcasted_iota(jnp.int32, acc.shape, 1)
        acc = jnp.where(blocks - 1 - row % blocks == slot // PB, acc, 0.0)
        v_re = jnp.sum(acc[:blocks], axis=0, keepdims=True)
        v_im = jnp.sum(acc[blocks:], axis=0, keepdims=True)
        row = lax.broadcasted_iota(jnp.int32, (8, W.shape[0]), 0)
        member = (row >> 1) + lax.div(here["gz"] * blocks, spacing) == sphere
        even = (row & 1) == 0
        v_one = jnp.where(member, jnp.where(even, v_re, v_im), 0.0)
        v_two = jnp.where(member, jnp.where(even, v_im, -v_re), 0.0)
        both = jnp.concatenate([v_one, v_two], 1) * (4.0 * math.pi / PTS)
        rest = both - both.astype(jnp.bfloat16).astype(jnp.float32)
        both = jnp.concatenate([both, rest], 0).astype(jnp.bfloat16)
        one = lax.dot_general(both, y_high, across, preferred_element_type=jnp.float32)
        two = lax.dot_general(both, y_low, across, preferred_element_type=jnp.float32)
        local = one[:8] + one[8:] + (two[:8] + two[8:])
        value = jnp.concatenate([local[:HELD], jnp.zeros((HELD, 128 - ROWS), jnp.float32)], 1)

    base = 0
    sends = []
    for phase, (me, count, peer, rising) in enumerate(groups):
        with jax.named_scope(f"reduce{phase}"):
            MINE[phase] = value
            copies = [
                pltpu.make_async_remote_copy(
                    src_ref=MINE.at[phase],
                    dst_ref=RED.at[base + me],
                    send_sem=ps_sem.at[phase],
                    recv_sem=pr_sem.at[phase],
                    device_id=rising(step),
                    device_id_type=LOGICAL,
                )
                for step in range(1, count)
            ]
            for copy in copies:
                copy.start()
            RED[base + me] = value
        everything = pltpu.make_async_remote_copy(
            src_ref=RED.at[pl.ds(base, count - 1)],
            dst_ref=RED.at[pl.ds(base, count - 1)],
            send_sem=ps_sem.at[phase],
            recv_sem=pr_sem.at[phase],
            device_id=peer(1),
            device_id_type=LOGICAL,
        )
        if phase == 0:
            with jax.named_scope("store_psi"):
                for c in range(2):
                    for x_index in range(cx):
                        psi_ref[c, x_index] = PS[c, x_index].astype(jnp.bfloat16)
        with jax.named_scope(f"gather{phase}"):
            everything.wait_recv()
            last = phase == len(groups) - 1
            sums = []
            for lot in range(counts["gz"] if last else 1):
                members = range(lot, count, counts["gz"]) if last else range(count)
                value = None
                for other in members:
                    value = RED[base + other] if value is None else value + RED[base + other]
                sums.append(value)
        sends.append(everything)
        base += count
    for s in range(SPHERES):
        total = None
        for lot in range(counts["gz"]):
            at = 2 * (s - lot * blocks // spacing)
            if 0 <= at < HELD:
                piece = sums[lot][at : at + 2, :MODES]
                total = piece if total is None else total + piece
        modes_ref[s] = total
    with jax.named_scope("tail"):
        for copy in sends:
            copy.wait_send()
        for at in range(0, len(moves), 2):
            (low, move, _, recv, _), (high, _, _, _, _) = moves[at], moves[at + 1]
            both = pltpu.make_async_remote_copy(
                src_ref=recv, dst_ref=recv, send_sem=send_sems[at // 2].at[0], recv_sem=load_sem.at[0],
                device_id=groups[0][2](1), device_id_type=LOGICAL,
            )

            @pl.when(jnp.logical_and(low, high))
            def _(both=both):
                both.wait_send()

            @pl.when(jnp.logical_xor(low, high))
            def _(move=move):
                move.wait_send()


def store_kernel(psi_ref, modes_ref, psi_out, modes_out, sem):
    small = pltpu.make_async_copy(modes_ref, modes_out, sem.at[1])
    small.start()
    whole = pltpu.make_async_copy(psi_ref, psi_out, sem.at[0])
    for c in range(psi_ref.shape[0]):
        for half in range(2):
            rows = pl.ds(half * (psi_ref.shape[1] // 2), psi_ref.shape[1] // 2)
            pltpu.make_async_copy(psi_ref.at[c, rows], psi_out.at[c, rows], sem.at[0]).start()
    whole.wait()
    small.wait()


def shards(counts, metric_pert, curvature, interp_weights, point_ids, theta, phi):
    _, cx, cy, cz = metric_pert.shape
    blocks = interp_weights.shape[2]
    points = theta.shape[0]
    vmem = pl.BlockSpec(memory_space=pltpu.VMEM)
    anywhere = pl.BlockSpec(memory_space=pl.ANY)
    many = math.prod(counts.values())
    total = many if many <= DIRECT else counts["gx"] * counts["gy"] + counts["gz"]
    phases = 1 if many <= DIRECT else 2
    dma = pltpu.SemaphoreType.DMA
    f32 = jnp.float32
    table = build_table()
    psi, modes = pl.pallas_call(
        functools.partial(kernel, counts),
        out_shape=(
            pltpu.VMEM((2, cx, cy, cz), jnp.bfloat16),
            pltpu.VMEM((SPHERES, 2, MODES), f32),
        ),
        in_specs=[anywhere] * 7,
        out_specs=(vmem, vmem),
        scratch_shapes=[
            pltpu.VMEM((12, cx + 5, LO + cy + PITCH - 8, cz), f32),
            pltpu.VMEM((blocks * PB, BLK * BLK * BLK), jnp.bfloat16),
            pltpu.VMEM((blocks, PB), jnp.int32),
            pltpu.VMEM((points // 128, 128), f32),
            pltpu.VMEM((points // 128, 128), f32),
            pltpu.VMEM(table.shape, jnp.bfloat16),
            pltpu.VMEM((WAVES * blocks, 128), f32),
            pltpu.VMEM((9, cx, cy, cz), f32),
            pltpu.VMEM((9, 9, 16, cz), f32),
            pltpu.VMEM((2, 8, cz), f32),
            pltpu.VMEM((2 * blocks, BLK * BLK * BLK), jnp.bfloat16),
            pltpu.VMEM((2, cx, cy, cz), f32),
            pltpu.VMEM((2, 2, 2, cy, cz), f32),
            pltpu.VMEM((2, 2, 2, cy, cz), f32),
            pltpu.VMEM((2, 2, 2, cx, cz), f32),
            pltpu.VMEM((2, 2, 2, cx, cz), f32),
            pltpu.VMEM((2, 8, cz), f32),
            pltpu.VMEM((2, 2, 8, cz), f32),
            pltpu.VMEM((total, HELD, 128), f32),
            pltpu.VMEM((2, HELD, 128), f32),
            dma((6,)), dma((1,)), dma((2,)), dma((1,)), dma((2,)), dma((1,)), dma((2,)),
            dma((phases,)), dma((phases,)),
        ],
        compiler_params=pltpu.CompilerParams(
            collective_id=0, has_side_effects=True, vmem_limit_bytes=60 * 1024 * 1024
        ),
    )(
        metric_pert,
        curvature,
        interp_weights.reshape(blocks * PB, BLK * BLK * BLK),
        point_ids.reshape(blocks, PB),
        theta.reshape(points // 128, 128),
        phi.reshape(points // 128, 128),
        jnp.asarray(table),
    )
    return pl.pallas_call(
        store_kernel,
        out_shape=(
            jax.ShapeDtypeStruct(psi.shape, psi.dtype),
            jax.ShapeDtypeStruct(modes.shape, modes.dtype),
        ),
        in_specs=[vmem, vmem],
        out_specs=(anywhere, anywhere),
        scratch_shapes=[dma((2,))],
        compiler_params=pltpu.CompilerParams(vmem_limit_bytes=1024 * 1024),
    )(psi, modes)


def solution(mesh):
    in_specs = (
        P(None, "gx", "gy", "gz"),
        P(None, "gx", "gy", "gz"),
        P("gx", "gy", "gz", None, None),
        P("gx", "gy", "gz", None),
        P(),
        P(),
    )
    out_specs = (P(None, "gx", "gy", "gz"), P())
    counts = {axis: mesh.shape[axis] for axis in AXES}
    return jax.shard_map(
        functools.partial(shards, counts), mesh=mesh, in_specs=in_specs, out_specs=out_specs, check_vma=False
    )
```
